256 devices in a mesh: blk: 32 (over x, z), sub: 8 (over y, core).
Axes of the slice: x: 4, y: 4, z: 8, core: 2. Of those that a mesh axis runs over, the one named last changes fastest.
Arguments:
- features: float32 [131072, 128], P(('blk', 'sub')), may hold values from -6 to 6
- weight: float32 [128, 128], replicated, may hold values from -0.5 to 0.5
- bias: float32 [128], replicated, may hold values from -3 to 3
- adj_tiles: float32 [16384, 128, 128], P(('blk', 'sub')), may hold values from 0 to 0.046875
- tile_rows: int32 [16384], P(('blk', 'sub')), may hold values from 0 to 1023, as said below
- tile_cols: int32 [16384], P(('blk', 'sub')), may hold values from 0 to 1023, as said below
- tile_counts: int32 [8192], P(('blk', 'sub')), may hold values from 0 to 2, as said below
- cotangent: float32 [131072, 128], P(('blk', 'sub')), may hold values from -6 to 6
Outputs:
- activation: float32 [131072, 128], P(('blk', 'sub'))
- grad_features: float32 [131072, 128], P(('blk', 'sub'))
- grad_weight: float32 [128, 128], replicated
- grad_bias: float32 [128], replicated
The draws below stay inside these ranges and needn't reach their ends.
Inputs may be any that keep to these rules, and one draw needn't show every extreme that they name: `tile_rows`: a slot's row block is one of the 32 blocks of the 8 devices that share the holding device's blk index. `tile_cols`: slot k of a device has its column block in group k // 2, the 32 blocks of the devices with blk index k // 2. `tile_counts`: the live slots of a group are its first ones; some device has all slots live in every draw.
All inputs are finite; a program needn't handle non-finite values.
Results may differ from the reference program's by a relative error of at most 0.00023.
Values sent between devices are 32-bit elements; how exact they have to be, the bound alone decides.
A program may use at most 128 MiB of HBM per device.

```python
import math
import jax
import jax.numpy as jnp
from jax import lax

FEAT = 128
BS = 128
CAP = 2
GROUP_BLOCKS = 32
SLOTS = 64
NODES = 131072
TILES = 16384
N_BLK = 32
N_SUB = 8
DEVICES = 256


def draw_tile_rows(key, part):
    index = jnp.arange(TILES, dtype=jnp.int32)
    group = index // SLOTS // N_SUB
    offset = jax.random.randint(jax.random.fold_in(key, 11), (TILES,), 0, GROUP_BLOCKS)
    return (group * GROUP_BLOCKS + offset).astype(jnp.int32)


def draw_tile_cols(key, part):
    index = jnp.arange(TILES, dtype=jnp.int32)
    group = index % SLOTS // CAP
    offset = jax.random.randint(jax.random.fold_in(key, 23), (TILES,), 0, GROUP_BLOCKS)
    return (group * GROUP_BLOCKS + offset).astype(jnp.int32)


def draw_tile_counts(key, part):
    index = jnp.arange(DEVICES * N_BLK, dtype=jnp.int32)
    device = index // N_BLK
    levels = jax.random.randint(jax.random.fold_in(key, 37), (DEVICES,), 0, 4)
    busy = (levels == 0) | (jnp.arange(DEVICES, dtype=jnp.int32) == 0)
    spread = jax.random.randint(jax.random.fold_in(key, 41), (DEVICES * N_BLK,), 0, CAP + 1)
    return jnp.where(busy[device], CAP, spread).astype(jnp.int32)


def block_scale(key, extent, split, least, high):
    def one(axis_at, shards_of):
        heights = jax.random.uniform(jax.random.fold_in(jax.random.fold_in(key, 6), axis_at), (shards_of,), jnp.float32, least / len(split), high / len(split))
        return jnp.repeat(jnp.exp(heights), extent[axis_at] // shards_of).reshape((-1,) + (1,) * (len(extent) - axis_at - 1))

    loudness = one(*split[0])
    for cut in split[1:]:
        loudness = loudness * one(*cut)
    return loudness


def noise(stream_key, shape, scale, reach, split=(), kind=jnp.bfloat16):
    values = scale * jax.random.normal(stream_key, shape, jnp.float32)
    if split:
        values = values * block_scale(stream_key, shape, split, -0.22, 0.18)
    return jnp.clip(values, -reach, reach).astype(kind)


def setup_inputs(seed: int = 0) -> dict:
    seeds = jax.random.split(jax.random.key(seed), 9)
    features = noise(seeds[0], (NODES, FEAT), 1.0, 6.0, ((0, 256),), jnp.float32)
    weight = noise(seeds[1], (FEAT, FEAT), FEAT ** -0.5, 0.5, (), jnp.float32)
    bias = noise(seeds[2], (FEAT,), 0.5, 3.0, (), jnp.float32)
    adj_tiles = jnp.clip(0.046875 * jax.random.uniform(seeds[3], (TILES, BS, BS), jnp.float32) ** block_scale(seeds[3], (TILES, BS, BS), ((0, 256),), -0.2, 0.2), 0.0, 0.046875)
    tile_rows = draw_tile_rows(jax.random.fold_in(seeds[8], 71), 0)
    tile_cols = draw_tile_cols(jax.random.fold_in(seeds[8], 71), 0)
    tile_counts = draw_tile_counts(jax.random.fold_in(seeds[8], 71), 0)
    cotangent = noise(seeds[7], (NODES, FEAT), 1.0, 6.0, ((0, 256),), jnp.float32)
    return dict(features=features, weight=weight, bias=bias, adj_tiles=adj_tiles, tile_rows=tile_rows, tile_cols=tile_cols, tile_counts=tile_counts, cotangent=cotangent)


def aggregate(values, adj_tiles, tile_rows, tile_cols, tile_counts):
    width = values.shape[1]
    blocked = values.reshape(-1, BS, width)
    slot_ids = jnp.arange(SLOTS, dtype=jnp.int32)
    counts_view = tile_counts.reshape(DEVICES, N_BLK)
    alive = ((slot_ids % CAP)[None, :] < counts_view[:, slot_ids // CAP]).astype(values.dtype)
    tiles_view = adj_tiles.reshape(DEVICES, SLOTS, BS, BS)
    rows_view = tile_rows.reshape(DEVICES, SLOTS)
    cols_view = tile_cols.reshape(DEVICES, SLOTS)

    def one_device(summed, pieces):
        tiles_here, rows_here, cols_here, alive_here = pieces
        masked = tiles_here * alive_here[:, None, None]
        pulled = jnp.einsum('kij,kjf->kif', masked, blocked[cols_here], precision=lax.Precision.HIGHEST)
        pushed = jnp.einsum('kji,kjf->kif', masked, blocked[rows_here], precision=lax.Precision.HIGHEST)
        summed = summed.at[rows_here].add(pulled)
        summed = summed.at[cols_here].add(pushed)
        return (summed, None)
    start = jnp.zeros(blocked.shape, values.dtype)
    summed, _ = lax.scan(one_device, start, (tiles_view, rows_view, cols_view, alive))
    return summed.reshape(values.shape)

def reference(features, weight, bias, adj_tiles, tile_rows, tile_cols, tile_counts, cotangent):
    scale = 1.0 / math.sqrt(NODES)
    mixed = jnp.dot(features, weight, precision=lax.Precision.HIGHEST)
    pre = aggregate(mixed, adj_tiles, tile_rows, tile_cols, tile_counts) + bias
    sigma = jax.nn.sigmoid(pre)
    activation = pre * sigma
    grad_pre = cotangent * sigma * (1.0 + pre * (1.0 - sigma))
    grad_mixed = aggregate(grad_pre, adj_tiles, tile_rows, tile_cols, tile_counts)
    grad_features = jnp.dot(grad_mixed, weight.T, precision=lax.Precision.HIGHEST)
    grad_weight = jnp.dot(features.T, grad_mixed, precision=lax.Precision.HIGHEST) * scale
    grad_bias = lax.optimization_barrier(jnp.sum(grad_pre, axis=0)) * scale
    return (activation, grad_features, grad_weight, grad_bias)
```

```python
import functools
import math

import jax
import jax.numpy as jnp
from jax import lax
from jax.experimental import pallas as pl
from jax.experimental.pallas import tpu as pltpu
from jax.sharding import Mesh
from jax.sharding import PartitionSpec as P

CAP = 2
MESH = pl.DeviceIdType.MESH
AX, AZ, AY, AC = "blk_0", "blk_1", "sub_0", "sub_1"
ALL = (AX, AZ, AY, AC)
BLK = (AX, AZ)
F32 = jnp.float32


def copy_to(src, dst, sends, recvs, at, where):
    return pltpu.make_async_remote_copy(
        src_ref=src,
        dst_ref=dst,
        send_sem=sends.at[at],
        recv_sem=recvs.at[at],
        device_id=where,
        device_id_type=MESH,
    )


def greet(places):
    barrier = pltpu.get_barrier_semaphore()
    for place in places:
        pl.semaphore_signal(barrier, inc=1, device_id=place, device_id_type=MESH)
    pl.semaphore_wait(barrier, len(places))


def visiting_order(count):
    order = [0]
    for step in range(1, count // 2 + 1):
        order.append(step)
        if count - step > count // 2:
            order.append(count - step)
    return order


def pull_kernel(sizes, wanted, own_ref, out_ref, *scratch):
    nx, nz, ny = sizes
    groups = scratch[:nz]
    picks, relays, kept = scratch[nz : nz + 3]
    zs, zr, ys, yr, cs, cr, xs, xr, ls = scratch[nz + 3 :]
    own = own_ref.shape[0]
    half = own // 2
    x, z, y, c = (lax.axis_index(a) for a in (AX, AZ, AY, AC))
    east, west = {AX: (x + 1) % nx}, {AX: (x + nx - 1) % nx}
    up, down = {AZ: (z + 1) % nz}, {AZ: (z + nz - 1) % nz}
    fore, back = {AY: (y + 1) % ny}, {AY: (y + ny - 1) % ny}
    mate = {AC: 1 - c}

    def part(j, away, core, first=0, count=own):
        line = (y + away + ny) % ny
        return groups[j].at[pl.ds((line * 2 + core) * own + first, count)]

    def mine(j):
        return own_ref if j == 0 else part(j, 0, c)

    def along_z(j):
        if j <= nz // 2:
            return copy_to(mine(j - 1), part(j, 0, c), zs, zr, j, up)
        return copy_to(mine((j + 1) % nz), part(j, 0, c), zs, zr, j, down)

    def along_y(j, kind):
        if kind == 0:
            return copy_to(mine(j), part(j, 0, c), ys, yr, (j, 0), fore)
        if kind == 1:
            return copy_to(mine(j), part(j, 0, c), ys, yr, (j, 1), back)
        if kind == 2:
            piece = part(j, -1, c, 0, half)
            return copy_to(piece, piece, ys, yr, (j, 2), fore)
        piece = part(j, 1, c, half, half)
        return copy_to(piece, piece, ys, yr, (j, 3), back)

    def landed_y(j, kind):
        if kind == 0:
            piece = part(j, -1, c)
        elif kind == 1:
            piece = part(j, 1, c)
        elif kind == 2:
            piece = part(j, 2, c, 0, half)
        else:
            piece = part(j, 2, c, half, half)
        copy_to(piece, piece, ys, yr, (j, kind), fore).wait_recv()

    def to_mate(j, kind):
        away = (0, -1, 1, 2)[kind]
        source = mine(j) if kind == 0 else part(j, away, c)
        return copy_to(source, part(j, away, c), cs, cr, (j, kind), mate)

    def landed_mate(j, kind):
        piece = part(j, (0, -1, 1, 2)[kind], 1 - c)
        copy_to(piece, piece, cs, cr, (j, kind), mate).wait_recv()

    def far(j):
        return (z + nz - j) % nz

    def line(away, j):
        return ((x + away + nx) % nx) * nz + far(j)

    def along_x(j, kind):
        if kind == 0:
            return copy_to(picks.at[j, pl.ds(0, 4)], out_ref.at[line(0, j)], xs, xr, (j, 0), east)
        if kind == 1:
            return copy_to(picks.at[j, pl.ds(4, 4)], out_ref.at[line(0, j)], xs, xr, (j, 1), west)
        if kind == 2:
            return copy_to(picks.at[j, pl.ds(8, 2)], relays.at[j, 0], xs, xr, (j, 2), east)
        if kind == 3:
            return copy_to(picks.at[j, pl.ds(10, 2)], relays.at[j, 1], xs, xr, (j, 3), west)
        if kind == 4:
            return copy_to(relays.at[j, 0], out_ref.at[line(-1, j), pl.ds(0, 2)], xs, xr, (j, 4), east)
        return copy_to(relays.at[j, 1], out_ref.at[line(1, j), pl.ds(2, 2)], xs, xr, (j, 5), west)

    def landed_x(j, kind):
        if kind == 0:
            piece = out_ref.at[line(-1, j)]
        elif kind == 1:
            piece = out_ref.at[line(1, j)]
        elif kind in (2, 3):
            piece = relays.at[j, kind - 2]
        elif kind == 4:
            piece = out_ref.at[line(2, j), pl.ds(0, 2)]
        else:
            piece = out_ref.at[line(2, j), pl.ds(2, 2)]
        copy_to(piece, piece, xs, xr, (j, kind), east).wait_recv()

    def keep(j):
        return pltpu.make_async_copy(kept.at[j], out_ref.at[line(0, j)], ls.at[j])

    order = visiting_order(nz)

    def spread(j):
        if j:
            along_z(j).wait_recv()
        if j == 0:
            along_z(1).start()
            if nz - 1 > nz // 2:
                along_z(nz - 1).start()
        elif j < nz // 2:
            along_z(j + 1).start()
        elif j > nz // 2 + 1:
            along_z(j - 1).start()
        along_y(j, 0).start()
        along_y(j, 1).start()
        to_mate(j, 0).start()

    def pass_on(j):
        landed_y(j, 0)
        along_y(j, 2).start()
        landed_y(j, 1)
        along_y(j, 3).start()
        to_mate(j, 1).start()
        to_mate(j, 2).start()
        landed_y(j, 2)
        landed_y(j, 3)
        to_mate(j, 3).start()

    def pick(j):
        for kind in range(4):
            landed_mate(j, kind)

        def asked(away, slot):
            return wanted[(((x + away) % nx) * nz + far(j)) * 4 + slot]

        def one(slot, carry):
            picks[j, slot] = groups[j][asked(1, slot)]
            picks[j, 4 + slot] = groups[j][asked(nx - 1, slot)]
            picks[j, 8 + slot] = groups[j][asked(2, slot)]
            kept[j, slot] = groups[j][asked(0, slot)]
            return carry

        lax.fori_loop(0, 4, one, 0)

    def answer(j):
        for kind in (2, 3, 0, 1):
            along_x(j, kind).start()
        keep(j).start()

    def relay(j):
        for kind in (2, 3):
            landed_x(j, kind)
            along_x(j, kind + 2).start()

    greet((east, west, up, down, fore, back, mate))
    spread(order[0])
    groups[0][pl.ds((y * 2 + c) * own, own)] = own_ref[...]
    spread(order[1])
    for n, j in enumerate(order):
        pass_on(j)
        pick(j)
        if n + 2 < nz:
            spread(order[n + 2])
        if n:
            relay(order[n - 1])
        answer(j)
    relay(order[-1])
    for j in order:
        for kind in (0, 1, 4, 5):
            landed_x(j, kind)
        keep(j).wait()
        if j:
            along_z(j).wait_send()
        for kind in range(4):
            along_y(j, kind).wait_send()
            to_mate(j, kind).wait_send()
        for kind in range(6):
            along_x(j, kind).wait_send()


def pull(sizes, wanted, value):
    nx, nz, ny = sizes
    own, rows, width = value.shape
    block = (rows, width)
    dma = pltpu.SemaphoreType.DMA
    return pl.pallas_call(
        functools.partial(pull_kernel, sizes),
        out_shape=jax.ShapeDtypeStruct((nx * nz, 4, *block), F32),
        in_specs=[
            pl.BlockSpec(memory_space=pltpu.SMEM),
            pl.BlockSpec(memory_space=pltpu.VMEM),
        ],
        out_specs=pl.BlockSpec(memory_space=pl.ANY),
        scratch_shapes=[pltpu.VMEM((ny * 2 * own, *block), F32) for _ in range(nz)]
        + [
            pltpu.VMEM((nz, 12, *block), F32),
            pltpu.VMEM((nz, 2, 2, *block), F32),
            pltpu.VMEM((nz, 4, *block), F32),
            dma((nz,)),
            dma((nz,)),
            dma((nz, 4)),
            dma((nz, 4)),
            dma((nz, 4)),
            dma((nz, 4)),
            dma((nz, 6)),
            dma((nz, 6)),
            dma((nz,)),
        ],
        compiler_params=pltpu.CompilerParams(
            collective_id=0, has_side_effects=True, vmem_limit_bytes=48 * 2**20
        ),
        cost_estimate=pl.CostEstimate(
            flops=20_000_000_000, bytes_accessed=17_000_000, transcendentals=0
        ),
        name="pull",
    )(wanted, value)


def scatter_kernel(ny, sums, out_ref, mated, total, early, late, cs, cr, ys, yr):
    own = out_ref.shape[0]
    half = own // 2
    y, c = lax.axis_index(AY), lax.axis_index(AC)
    fore, back, mate = {AY: (y + 1) % ny}, {AY: (y + ny - 1) % ny}, {AC: 1 - c}

    def at(away, core):
        return pl.ds((((y + away) % ny) * 2 + core) * own, own)

    def over(k):
        return copy_to(sums.at[at(k, 1 - c)], mated.at[k], cs, cr, k, mate)

    early_fore = copy_to(total.at[2, pl.ds(0, half)], early.at[0], ys, yr, 0, fore)
    early_back = copy_to(total.at[2, pl.ds(half, half)], early.at[1], ys, yr, 1, back)
    late_fore = copy_to(total.at[1], late.at[0], ys, yr, 2, fore)
    late_back = copy_to(total.at[3], late.at[1], ys, yr, 3, back)
    greet((fore, back, mate))
    for k in (2, 1, 3, 0):
        over(k).start()
    for k in (2, 1, 3, 0):
        over(k).wait_recv()
        total[k] = sums[at(k, c)] + mated[k]
        if k == 1:
            early_fore.start()
            early_back.start()
    early_fore.wait_recv()
    total[1, pl.ds(0, half)] = total[1, pl.ds(0, half)] + early[0]
    early_back.wait_recv()
    total[3, pl.ds(half, half)] = total[3, pl.ds(half, half)] + early[1]
    late_fore.start()
    late_back.start()
    late_fore.wait_recv()
    late_back.wait_recv()
    out_ref[...] = total[0] + late[0] + late[1]
    for k in range(4):
        over(k).wait_send()
    for copy in (early_fore, early_back, late_fore, late_back):
        copy.wait_send()


def scatter(ny, sums):
    count, rows, width = sums.shape
    own = count // (2 * ny)
    dma = pltpu.SemaphoreType.DMA
    piece = (own, rows, width)
    return pl.pallas_call(
        functools.partial(scatter_kernel, ny),
        out_shape=jax.ShapeDtypeStruct(piece, F32),
        in_specs=[pl.BlockSpec(memory_space=pltpu.VMEM)],
        out_specs=pl.BlockSpec(memory_space=pltpu.VMEM),
        scratch_shapes=[
            pltpu.VMEM((4, *piece), F32),
            pltpu.VMEM((4, *piece), F32),
            pltpu.VMEM((2, own // 2, rows, width), F32),
            pltpu.VMEM((2, *piece), F32),
            dma((4,)),
            dma((4,)),
            dma((4,)),
            dma((4,)),
        ],
        compiler_params=pltpu.CompilerParams(
            collective_id=1, has_side_effects=True, vmem_limit_bytes=16 * 2**20
        ),
        cost_estimate=pl.CostEstimate(
            flops=2_000_000_000, bytes_accessed=2_000_000, transcendentals=0
        ),
        name="scatter",
    )(sums)


def halves(value):
    high = value.astype(jnp.bfloat16)
    return high, (value - high.astype(F32)).astype(jnp.bfloat16)


def product(tile, value, flipped):
    dims = (((0 if flipped else 1,), (0,)), ((), ()))
    tile_high, tile_low = halves(tile)
    high, low = halves(value)

    def dot(a, b):
        return lax.dot_general(a, b, dims, preferred_element_type=F32)

    return dot(tile_high, high) + (dot(tile_high, low) + dot(tile_low, high))


def apply_kernel(step, target, alive, near, moved, values, sums):
    first = pl.program_id(0) * step

    @pl.when(first == 0)
    def _():
        sums[...] = jnp.zeros_like(sums)

    for g in range(step):
        for slot in range(4):
            place = (first + g) * 4 + slot
            block = (near if slot < 2 else moved)[g, slot % 2]

            @pl.when(alive[place] > 0)
            def _(block=block, place=place, g=g, slot=slot):
                sums[target[place]] += product(block, values[g, slot], slot >= 2)


def apply(group_size, target, alive, near, moved, values):
    count, _, rows, width = values.shape
    step = 2
    tiles = pl.BlockSpec((step, 2, rows, rows), lambda n, *_: (n, 0, 0, 0))
    return pl.pallas_call(
        functools.partial(apply_kernel, step),
        out_shape=jax.ShapeDtypeStruct((group_size, rows, width), F32),
        grid_spec=pltpu.PrefetchScalarGridSpec(
            num_scalar_prefetch=2,
            grid=(count // step,),
            in_specs=[
                tiles,
                tiles,
                pl.BlockSpec((step, 4, rows, width), lambda n, *_: (n, 0, 0, 0)),
            ],
            out_specs=pl.BlockSpec((group_size, rows, width), lambda n, *_: (0, 0, 0)),
        ),
        compiler_params=pltpu.CompilerParams(vmem_limit_bytes=24 * 2**20),
        cost_estimate=pl.CostEstimate(
            flops=count * 4 * 6 * rows * rows * width,
            bytes_accessed=19_000_000,
            transcendentals=0,
        ),
        name="apply",
    )(target, alive, near, moved, values)


def exchanged(value, axis):
    return lax.all_to_all(value, axis, 0, 0, tiled=True)


def far_sum(pieces, axis):
    return exchanged(pieces, axis).sum(axis=0)


def for_each(value, axis):
    peers = lax.axis_size(axis)
    return exchanged(jnp.broadcast_to(value[None], (peers, *value.shape)), axis)


def param_sum(vector):
    blocks, subs = lax.axis_size(BLK), lax.axis_size((AY, AC))
    spare = -vector.shape[0] % (blocks * subs)
    padded = jnp.concatenate([vector, jnp.zeros((spare,), F32)]).reshape(blocks, subs, -1)
    near = far_sum(padded.swapaxes(0, 1), (AY, AC))
    done = far_sum(near, BLK)
    line = for_each(done, BLK)
    whole = for_each(line, (AY, AC))
    return whole.swapaxes(0, 1).reshape(-1)[: vector.shape[0]]


def body(features, weight, bias, adj_tiles, tile_rows, tile_cols, tile_counts, cotangent):
    nx, nz, ny = (lax.axis_size(a) for a in (AX, AZ, AY))
    sizes = (nx, nz, ny)
    blocks = nx * nz
    rows, width = adj_tiles.shape[1], features.shape[1]
    own = features.shape[0] // rows
    group_size = own * ny * 2
    group = lax.axis_index(BLK)
    scale = 1.0 / math.sqrt(features.shape[0] * blocks * ny * 2)
    slots = jnp.arange(blocks * CAP, dtype=jnp.int32)
    alive = (slots % CAP < tile_counts[slots // CAP]).astype(jnp.int32)
    row_local = tile_rows - group * group_size
    col_local = tile_cols - slots // CAP * group_size
    near = adj_tiles.reshape(blocks, CAP, rows, rows)
    moved = exchanged(near, BLK)

    by_group = (blocks, CAP)
    told = exchanged(
        jnp.concatenate([col_local.reshape(by_group), alive.reshape(by_group)], axis=1), BLK
    )
    direct = exchanged(col_local.reshape(nx, nz, CAP), AX)
    turned = exchanged(row_local.reshape(nx, nz, CAP).swapaxes(0, 1), AZ).swapaxes(0, 1)
    wanted = jnp.concatenate([direct, turned], axis=2).reshape(-1)
    target = jnp.concatenate([row_local.reshape(by_group), told[:, :CAP]], axis=1).reshape(-1)
    live = jnp.concatenate([alive.reshape(by_group), told[:, CAP:]], axis=1).reshape(-1)

    def aggregate(value):
        fetched = pull(sizes, wanted, value.reshape(own, rows, width))
        sums = apply(group_size, target, live, near, moved, fetched)
        return scatter(ny, sums).reshape(value.shape)

    dot = functools.partial(jnp.dot, precision=lax.Precision.HIGHEST)
    spread = aggregate(features)
    pre = dot(spread, weight) + bias
    sigma = jax.nn.sigmoid(pre)
    activation = pre * sigma
    grad_pre = cotangent * sigma * (1.0 + pre * (1.0 - sigma))
    vector = jnp.concatenate(
        [(dot(spread.T, grad_pre) * scale).reshape(-1), jnp.sum(grad_pre, axis=0) * scale]
    )
    params = param_sum(vector)
    grad_mixed = aggregate(grad_pre)
    grad_features = dot(grad_mixed, weight.T)
    grad_weight = params[: weight.size].reshape(weight.shape)
    return (activation, grad_features, grad_weight, params[weight.size :])


def solution(mesh):
    finer = Mesh(mesh.devices.reshape(4, 8, 4, 2), ALL)
    return jax.shard_map(
        body,
        mesh=finer,
        in_specs=(
            P(ALL, None),
            P(),
            P(),
            P(ALL, None, None),
            P(ALL),
            P(ALL),
            P(ALL),
            P(ALL, None),
        ),
        out_specs=(P(ALL, None), P(ALL, None), P(), P()),
        check_vma=False,
    )
```

```python
import functools
import math

import jax
import jax.numpy as jnp
from jax import lax
from jax.experimental import pallas as pl
from jax.experimental.pallas import tpu as pltpu
from jax.sharding import Mesh
from jax.sharding import PartitionSpec as P

CAP = 2
MESH = pl.DeviceIdType.MESH
AX, AZ, AY, AC = "blk_0", "blk_1", "sub_0", "sub_1"
ALL = (AX, AZ, AY, AC)
BLK = (AX, AZ)
F32 = jnp.float32


def copy_to(src, dst, sends, recvs, at, where):
    return pltpu.make_async_remote_copy(
        src_ref=src,
        dst_ref=dst,
        send_sem=sends.at[at],
        recv_sem=recvs.at[at],
        device_id=where,
        device_id_type=MESH,
    )


def greet(places):
    barrier = pltpu.get_barrier_semaphore()
    for place in places:
        pl.semaphore_signal(barrier, inc=1, device_id=place, device_id_type=MESH)
    pl.semaphore_wait(barrier, len(places))


def visiting_order(count):
    order = [0]
    for step in range(1, count // 2 + 1):
        order.append(step)
        if count - step > count // 2:
            order.append(count - step)
    return order


def pull_kernel(sizes, first, fuse, *refs):
    nx, nz, ny = sizes
    refs = list(refs)

    def take(count):
        taken, refs[:count] = refs[:count], []
        return taken

    if first:
        ids_ref, own_ref, near_ref = take(3)
        out_ref, moved_ref, told_ref = take(3)
    else:
        asks, own_ref, near_ref, moved_ref = take(4)
        (out_ref,) = take(1)
    groups = take(nz)
    picks, relays, landing = take(3)
    zs, zr, ys, yr, cs, cr, xs, xr, ls = take(9)
    if first or fuse:
        (moved,) = take(1)
    if fuse:
        near, = take(1)
    if first:
        passing, tossed, table, asks = take(4)
        ts, tr, us, ur, js, jr, ms = take(7)
    own = own_ref.shape[0]
    half = own // 2
    x, z, y, c = (lax.axis_index(a) for a in (AX, AZ, AY, AC))
    east, west = {AX: (x + 1) % nx}, {AX: (x + nx - 1) % nx}
    up, down = {AZ: (z + 1) % nz}, {AZ: (z + nz - 1) % nz}
    fore, back = {AY: (y + 1) % ny}, {AY: (y + ny - 1) % ny}
    mate = {AC: 1 - c}

    def part(j, away, core, start=0, count=own):
        line = (y + away + ny) % ny
        return groups[j].at[pl.ds((line * 2 + core) * own + start, count)]

    def mine(j):
        return own_ref if j == 0 else part(j, 0, c)

    def along_z(j):
        if j <= nz // 2:
            return copy_to(mine(j - 1), part(j, 0, c), zs, zr, j, up)
        return copy_to(mine((j + 1) % nz), part(j, 0, c), zs, zr, j, down)

    def along_y(j, kind):
        if kind == 0:
            return copy_to(mine(j), part(j, 0, c), ys, yr, (j, 0), fore)
        if kind == 1:
            return copy_to(mine(j), part(j, 0, c), ys, yr, (j, 1), back)
        if kind == 2:
            piece = part(j, -1, c, 0, half)
            return copy_to(piece, piece, ys, yr, (j, 2), fore)
        piece = part(j, 1, c, half, half)
        return copy_to(piece, piece, ys, yr, (j, 3), back)

    def landed_y(j, kind):
        if kind == 0:
            piece = part(j, -1, c)
        elif kind == 1:
            piece = part(j, 1, c)
        elif kind == 2:
            piece = part(j, 2, c, 0, half)
        else:
            piece = part(j, 2, c, half, half)
        copy_to(piece, piece, ys, yr, (j, kind), fore).wait_recv()

    def to_mate(j, kind):
        away = (0, -1, 1, 2)[kind]
        source = mine(j) if kind == 0 else part(j, away, c)
        return copy_to(source, part(j, away, c), cs, cr, (j, kind), mate)

    def landed_mate(j, kind):
        piece = part(j, (0, -1, 1, 2)[kind], 1 - c)
        copy_to(piece, piece, cs, cr, (j, kind), mate).wait_recv()

    def far(j):
        return (z + nz - j) % nz

    def row(away):
        return (x + away + nx) % nx

    def along_x(j, kind):
        if kind == 0:
            return copy_to(picks.at[j, pl.ds(0, 4)], landing.at[x, far(j)], xs, xr, (j, 0), east)
        if kind == 1:
            return copy_to(picks.at[j, pl.ds(4, 4)], landing.at[x, far(j)], xs, xr, (j, 1), west)
        if kind == 2:
            return copy_to(picks.at[j, pl.ds(8, 2)], relays.at[j, 0], xs, xr, (j, 2), east)
        if kind == 3:
            return copy_to(picks.at[j, pl.ds(10, 2)], relays.at[j, 1], xs, xr, (j, 3), west)
        if kind == 4:
            place = landing.at[row(-1), far(j), pl.ds(0, 2)]
            return copy_to(relays.at[j, 0], place, xs, xr, (j, 4), east)
        place = landing.at[row(1), far(j), pl.ds(2, 2)]
        return copy_to(relays.at[j, 1], place, xs, xr, (j, 5), west)

    def landed_x(j, kind):
        if kind == 0:
            piece = landing.at[row(-1), far(j)]
        elif kind == 1:
            piece = landing.at[row(1), far(j)]
        elif kind in (2, 3):
            piece = relays.at[j, kind - 2]
        elif kind == 4:
            piece = landing.at[row(2), far(j), pl.ds(0, 2)]
        else:
            piece = landing.at[row(2), far(j), pl.ds(2, 2)]
        copy_to(piece, piece, xs, xr, (j, kind), east).wait_recv()

    def tiles_z(d):
        there = (z + d) % nz
        return copy_to(near_ref.at[:, there], passing.at[d], ts, tr, d, {AZ: there})

    def tiles_for(j, away):
        return near_ref.at[row(away), z] if j == 0 else passing.at[j, row(away)]

    def tiles_x(j, kind):
        if kind == 0:
            return copy_to(tiles_for(j, 1), moved.at[x, far(j)], us, ur, (j, 0), east)
        if kind == 1:
            return copy_to(tiles_for(j, -1), moved.at[x, far(j)], us, ur, (j, 1), west)
        if kind == 2:
            return copy_to(tiles_for(j, 2).at[0], tossed.at[j, 0], us, ur, (j, 2), east)
        if kind == 3:
            return copy_to(tiles_for(j, 2).at[1], tossed.at[j, 1], us, ur, (j, 3), west)
        if kind == 4:
            return copy_to(tossed.at[j, 0], moved.at[row(-1), far(j), 0], us, ur, (j, 4), east)
        return copy_to(tossed.at[j, 1], moved.at[row(1), far(j), 1], us, ur, (j, 5), west)

    def landed_tiles(j, kind):
        if kind == 0:
            piece = moved.at[row(-1), far(j)]
        elif kind == 1:
            piece = moved.at[row(1), far(j)]
        elif kind in (2, 3):
            piece = tossed.at[j, kind - 2]
        elif kind == 4:
            piece = moved.at[row(2), far(j), 0]
        else:
            piece = moved.at[row(2), far(j), 1]
        copy_to(piece, piece, us, ur, (j, kind), east).wait_recv()

    def ids_z(d):
        return copy_to(ids_ref, table.at[x, z], js, jr, d, {AZ: (z + d) % nz})

    def ids_x(d):
        return copy_to(table.at[x], table.at[x], js, jr, nz + d, {AX: (x + d) % nx})

    kept_tiles = lambda: pltpu.make_async_copy(near_ref.at[x, z], moved.at[x, z], ls.at[0])
    all_near = lambda: pltpu.make_async_copy(near_ref, near, ls.at[1])
    all_moved = lambda: pltpu.make_async_copy(moved_ref, moved, ls.at[2])
    all_asks = lambda: pltpu.make_async_copy(table, asks, ls.at[3])

    def results(j):
        return pltpu.make_async_copy(landing.at[:, far(j)], out_ref.at[:, far(j)], ls.at[4 + j])

    def moved_out(j):
        return pltpu.make_async_copy(moved.at[:, far(j)], moved_ref.at[:, far(j)], ms.at[j])

    order = visiting_order(nz)
    here = {0}

    def await_z(j):
        if j not in here:
            here.add(j)
            along_z(j).wait_recv()

    def z_step(k):
        for j, step in ((k, 1), (nz - k, -1)):
            ahead = j + step
            if k == 0:
                j, ahead = 0, (1 if step == 1 else nz - 1)
            if step == 1 and ahead > nz // 2 or step == -1 and ahead <= nz // 2:
                continue
            await_z(j)
            along_z(ahead).start()

    def tile_step(k):
        if first and k <= nz // 2:
            for d in sorted({k, nz - k}):
                tiles_z(d).start()

    def spread(j):
        await_z(j)
        along_y(j, 0).start()
        along_y(j, 1).start()
        to_mate(j, 0).start()

    def pass_on(j):
        landed_y(j, 0)
        along_y(j, 2).start()
        landed_y(j, 1)
        along_y(j, 3).start()
        to_mate(j, 1).start()
        to_mate(j, 2).start()
        landed_y(j, 2)
        landed_y(j, 3)
        to_mate(j, 3).start()

    def pick(j):
        for kind in range(4):
            landed_mate(j, kind)

        def asked(away, slot, late):
            line = row(away)
            if late:
                return asks[x, far(j), 0, (line * nz + z) * CAP + slot]
            return asks[line, z, 0, nx * nz * CAP + (x * nz + far(j)) * CAP + slot]

        def one(slot, carry):
            for late in range(2):
                place = late * CAP + slot
                picks[j, place] = groups[j][asked(1, slot, late)]
                picks[j, 4 + place] = groups[j][asked(-1, slot, late)]
                picks[j, 8 + place] = groups[j][asked(2, slot, late)]
                landing[x, far(j), place] = groups[j][asked(0, slot, late)]
            return carry

        lax.fori_loop(0, CAP, one, 0)

    def answer(j):
        for kind in (2, 3, 0, 1):
            along_x(j, kind).start()
        if first:
            if j:
                tiles_z(j).wait_recv()
                moved[x, far(j)] = passing[j, x]
            for kind in (2, 3, 0, 1):
                tiles_x(j, kind).start()

    def relay(j):
        for kind in (2, 3):
            landed_x(j, kind)
            along_x(j, kind + 2).start()
        if first:
            for kind in (2, 3):
                landed_tiles(j, kind)
                tiles_x(j, kind + 2).start()

    def finish(j):
        for kind in (0, 1, 4, 5):
            landed_x(j, kind)
            if first:
                landed_tiles(j, kind)
        if fuse:

            def one(line, carry):
                for slot in range(CAP):
                    value = landing[line, far(j), slot]
                    landing[line, far(j), slot] = product(near[line, far(j), slot], value, False)
                    value = landing[line, far(j), CAP + slot]
                    tile = moved[line, far(j), slot]
                    landing[line, far(j), CAP + slot] = product(tile, value, True)
                return carry

            lax.fori_loop(0, nx, one, 0)
        results(j).start()
        if first:
            moved_out(j).start()

    places = [east, west, up, down, fore, back, mate]
    if first:
        places += [{AX: (x + 2) % nx}] + [{AZ: (z + d) % nz} for d in range(2, nz - 1)]
    greet(places)
    if first:
        for d in range(1, nz):
            ids_z(d).start()
    z_step(0)
    spread(0)
    if first:
        kept_tiles().start()
        table[x, z] = ids_ref[...]
    elif fuse:
        all_moved().start()
    if fuse:
        all_near().start()
    groups[0][pl.ds((y * 2 + c) * own, own)] = own_ref[...]
    spread(order[1])
    z_step(1)
    if first:
        for d in range(1, nz):
            copy_to(table.at[x, far(d)], table.at[x, far(d)], js, jr, d, up).wait_recv()
        for d in range(1, nx):
            ids_x(d).start()
    for n, j in enumerate(order):
        pass_on(j)
        if n == 0:
            if first:
                kept_tiles().wait()
                for d in range(1, nx):
                    copy_to(table.at[row(-d)], table.at[row(-d)], js, jr, nz + d, east).wait_recv()
                all_asks().start()
                all_asks().wait()
            elif fuse:
                all_moved().wait()
            if fuse:
                all_near().wait()
        pick(j)
        if n + 2 < nz:
            spread(order[n + 2])
        if n + 2 < nz // 2:
            z_step(n + 2)
        if n == 2:
            for k in range(3, nz // 2 + 1):
                tile_step(k)
        elif n < 2:
            tile_step(n + 1)
        if n:
            relay(order[n - 1])
        answer(j)
        if n > 1:
            finish(order[n - 2])
    relay(order[-1])
    finish(order[-2])
    finish(order[-1])
    if first:
        told_ref[...] = table[...]
    for j in order:
        results(j).wait()
        if j:
            along_z(j).wait_send()
        for kind in range(4):
            along_y(j, kind).wait_send()
            to_mate(j, kind).wait_send()
        for kind in range(6):
            along_x(j, kind).wait_send()
        if first:
            moved_out(j).wait()
            for kind in range(6):
                tiles_x(j, kind).wait_send()
            if j:
                tiles_z(j).wait_send()
                ids_z(j).wait_send()
    if first:
        for d in range(1, nx):
            ids_x(d).wait_send()


FUSE = False


def pull(sizes, asks, value, near, moved=None):
    nx, nz, ny = sizes
    first = moved is None
    own, rows, width = value.shape
    block = (rows, width)
    dma = pltpu.SemaphoreType.DMA
    tiles = (nx, nz, CAP, rows, rows)
    values = (nx, nz, 2 * CAP, *block)
    anywhere, vmem = pl.BlockSpec(memory_space=pl.ANY), pl.BlockSpec(memory_space=pltpu.VMEM)
    smem = pl.BlockSpec(memory_space=pltpu.SMEM)
    out_shape = [jax.ShapeDtypeStruct(values, F32)]
    out_specs = [anywhere]
    in_specs = [smem, vmem, anywhere, anywhere]
    scratch = [pltpu.VMEM((ny * 2 * own, *block), F32) for _ in range(nz)] + [
        pltpu.VMEM((nz, 12, *block), F32),
        pltpu.VMEM((nz, 2, 2, *block), F32),
        pltpu.VMEM(values, F32),
        dma((nz,)),
        dma((nz,)),
        dma((nz, 4)),
        dma((nz, 4)),
        dma((nz, 4)),
        dma((nz, 4)),
        dma((nz, 6)),
        dma((nz, 6)),
        dma((4 + nz,)),
    ]
    operands = [asks, value, near, moved]
    if first or FUSE:
        scratch += [pltpu.VMEM(tiles, F32)]
    if FUSE:
        scratch += [pltpu.VMEM(tiles, F32)]
    if first:
        in_specs = [vmem, vmem, anywhere]
        operands = operands[:3]
        told = (nx, nz, *asks.shape)
        out_shape += [jax.ShapeDtypeStruct(tiles, F32), jax.ShapeDtypeStruct(told, jnp.int32)]
        out_specs += [anywhere, vmem]
        scratch += [
            pltpu.VMEM((nz, nx, CAP, rows, rows), F32),
            pltpu.VMEM((nz, 2, rows, rows), F32),
            pltpu.VMEM(told, jnp.int32),
            pltpu.SMEM(told, jnp.int32),
            dma((nz,)),
            dma((nz,)),
            dma((nz, 6)),
            dma((nz, 6)),
            dma((nz + nx,)),
            dma((nz + nx,)),
            dma((nz,)),
        ]
    elif not FUSE:
        in_specs, operands = in_specs[:3] + in_specs[3:], operands
    return pl.pallas_call(
        functools.partial(pull_kernel, sizes, first, FUSE),
        out_shape=out_shape,
        in_specs=in_specs,
        out_specs=out_specs,
        scratch_shapes=scratch,
        compiler_params=pltpu.CompilerParams(
            collective_id=0 if first else 2,
            has_side_effects=True,
            vmem_limit_bytes=58 * 2**20,
        ),
        cost_estimate=pl.CostEstimate(
            flops=20_000_000_000, bytes_accessed=17_000_000, transcendentals=0
        ),
        name="pull_first" if first else "pull_again",
    )(*operands)


def scatter_kernel(ny, sums, out_ref, mated, total, early, late, cs, cr, ys, yr):
    own = out_ref.shape[0]
    half = own // 2
    y, c = lax.axis_index(AY), lax.axis_index(AC)
    fore, back, mate = {AY: (y + 1) % ny}, {AY: (y + ny - 1) % ny}, {AC: 1 - c}

    def at(away, core):
        return pl.ds((((y + away) % ny) * 2 + core) * own, own)

    def over(k):
        return copy_to(sums.at[at(k, 1 - c)], mated.at[k], cs, cr, k, mate)

    early_fore = copy_to(total.at[2, pl.ds(0, half)], early.at[0], ys, yr, 0, fore)
    early_back = copy_to(total.at[2, pl.ds(half, half)], early.at[1], ys, yr, 1, back)
    late_fore = copy_to(total.at[1], late.at[0], ys, yr, 2, fore)
    late_back = copy_to(total.at[3], late.at[1], ys, yr, 3, back)
    greet((fore, back, mate))
    for k in (2, 1, 3, 0):
        over(k).start()
    for k in (2, 1, 3, 0):
        over(k).wait_recv()
        total[k] = sums[at(k, c)] + mated[k]
        if k == 1:
            early_fore.start()
            early_back.start()
    early_fore.wait_recv()
    total[1, pl.ds(0, half)] = total[1, pl.ds(0, half)] + early[0]
    early_back.wait_recv()
    total[3, pl.ds(half, half)] = total[3, pl.ds(half, half)] + early[1]
    late_fore.start()
    late_back.start()
    late_fore.wait_recv()
    late_back.wait_recv()
    out_ref[...] = total[0] + late[0] + late[1]
    for k in range(4):
        over(k).wait_send()
    for copy in (early_fore, early_back, late_fore, late_back):
        copy.wait_send()


def scatter(ny, sums):
    count, rows, width = sums.shape
    own = count // (2 * ny)
    dma = pltpu.SemaphoreType.DMA
    piece = (own, rows, width)
    return pl.pallas_call(
        functools.partial(scatter_kernel, ny),
        out_shape=jax.ShapeDtypeStruct(piece, F32),
        in_specs=[pl.BlockSpec(memory_space=pltpu.VMEM)],
        out_specs=pl.BlockSpec(memory_space=pltpu.VMEM),
        scratch_shapes=[
            pltpu.VMEM((4, *piece), F32),
            pltpu.VMEM((4, *piece), F32),
            pltpu.VMEM((2, own // 2, rows, width), F32),
            pltpu.VMEM((2, *piece), F32),
            dma((4,)),
            dma((4,)),
            dma((4,)),
            dma((4,)),
        ],
        compiler_params=pltpu.CompilerParams(
            collective_id=1, has_side_effects=True, vmem_limit_bytes=16 * 2**20
        ),
        cost_estimate=pl.CostEstimate(
            flops=2_000_000_000, bytes_accessed=2_000_000, transcendentals=0
        ),
        name="scatter",
    )(sums)


def halves(value):
    high = value.astype(jnp.bfloat16)
    return high, (value - high.astype(F32)).astype(jnp.bfloat16)


def product(tile, value, flipped):
    dims = (((0 if flipped else 1,), (0,)), ((), ()))
    tile_high, tile_low = halves(tile)
    high, low = halves(value)

    def dot(a, b):
        return lax.dot_general(a, b, dims, preferred_element_type=F32)

    return dot(tile_high, high) + (dot(tile_high, low) + dot(tile_low, high))


def apply_kernel(step, group, told, near, moved, values, sums):
    first = pl.program_id(0) * step
    count = pl.num_programs(0) * step * CAP
    me = group[0]

    @pl.when(first == 0)
    def _():
        sums[...] = jnp.zeros_like(sums)

    for g in range(step):
        for slot in range(4):
            block = (near if slot < CAP else moved)[g, slot % CAP]
            if slot < CAP:
                at = me * (4 * count) + (first + g) * CAP + slot
                alive, target = told[at + 2 * count], told[at]
            else:
                at = (first + g) * (4 * count) + me * CAP + slot - CAP
                alive, target = told[at + 2 * count], told[at + count]

            @pl.when(alive > 0)
            def _(block=block, target=target, g=g, slot=slot):
                sums[target] += product(block, values[g, slot], slot >= CAP)


def apply(group_size, group, told, near, moved, values):
    count, _, rows, width = values.shape
    step = 2
    tiles = pl.BlockSpec((step, 2, rows, rows), lambda n, *_: (n, 0, 0, 0))
    return pl.pallas_call(
        functools.partial(apply_kernel, step),
        out_shape=jax.ShapeDtypeStruct((group_size, rows, width), F32),
        grid_spec=pltpu.PrefetchScalarGridSpec(
            num_scalar_prefetch=2,
            grid=(count // step,),
            in_specs=[
                tiles,
                tiles,
                pl.BlockSpec((step, 4, rows, width), lambda n, *_: (n, 0, 0, 0)),
            ],
            out_specs=pl.BlockSpec((group_size, rows, width), lambda n, *_: (0, 0, 0)),
        ),
        compiler_params=pltpu.CompilerParams(vmem_limit_bytes=24 * 2**20),
        cost_estimate=pl.CostEstimate(
            flops=count * 4 * 6 * rows * rows * width,
            bytes_accessed=19_000_000,
            transcendentals=0,
        ),
        name="apply",
    )(group, told, near, moved, values)


def exchanged(value, axis):
    return lax.all_to_all(value, axis, 0, 0, tiled=True)


def far_sum(pieces, axis):
    return exchanged(pieces, axis).sum(axis=0)


def for_each(value, axis):
    peers = lax.axis_size(axis)
    return exchanged(jnp.broadcast_to(value[None], (peers, *value.shape)), axis)


def param_sum(vector):
    blocks, subs = lax.axis_size(BLK), lax.axis_size((AY, AC))
    spare = -vector.shape[0] % (blocks * subs)
    padded = jnp.concatenate([vector, jnp.zeros((spare,), F32)]).reshape(blocks, subs, -1)
    near = far_sum(padded.swapaxes(0, 1), (AY, AC))
    done = far_sum(near, BLK)
    line = for_each(done, BLK)
    whole = for_each(line, (AY, AC))
    return whole.swapaxes(0, 1).reshape(-1)[: vector.shape[0]]


def body(features, weight, bias, adj_tiles, tile_rows, tile_cols, tile_counts, cotangent):
    nx, nz, ny = (lax.axis_size(a) for a in (AX, AZ, AY))
    sizes = (nx, nz, ny)
    blocks = nx * nz
    rows, width = adj_tiles.shape[1], features.shape[1]
    own = features.shape[0] // rows
    group_size = own * ny * 2
    group = lax.axis_index(BLK)
    scale = 1.0 / math.sqrt(features.shape[0] * blocks * ny * 2)
    slots = jnp.arange(blocks * CAP, dtype=jnp.int32)
    alive = (slots % CAP < tile_counts[slots // CAP]).astype(jnp.int32)
    row_local = tile_rows - group * group_size
    col_local = tile_cols - slots // CAP * group_size
    ids = jnp.concatenate([row_local, col_local, alive, alive]).reshape(2, -1)
    near = adj_tiles.reshape(nx, nz, CAP, rows, rows)

    def paired(tiles):
        return tiles.reshape(blocks, CAP, rows, rows)

    def aggregate(value, asks, moved=None):
        pulled = pull(sizes, asks, value.reshape(own, rows, width), near, moved)
        if moved is None:
            fetched, moved, asks = pulled
        else:
            (fetched,) = pulled
        fetched = fetched.reshape(blocks, 2 * CAP, rows, width)
        me = group.astype(jnp.int32).reshape(1)
        sums = apply(group_size, me, asks.reshape(-1), paired(near), paired(moved), fetched)
        return scatter(ny, sums).reshape(value.shape), asks, moved

    dot = functools.partial(jnp.dot, precision=lax.Precision.HIGHEST)
    spread, asks, moved = aggregate(features, ids)
    pre = dot(spread, weight) + bias
    sigma = jax.nn.sigmoid(pre)
    activation = pre * sigma
    grad_pre = cotangent * sigma * (1.0 + pre * (1.0 - sigma))
    vector = jnp.concatenate(
        [(dot(spread.T, grad_pre) * scale).reshape(-1), jnp.sum(grad_pre, axis=0) * scale]
    )
    params = param_sum(vector)
    grad_mixed = aggregate(grad_pre, asks, moved)[0]
    grad_features = dot(grad_mixed, weight.T)
    grad_weight = params[: weight.size].reshape(weight.shape)
    return (activation, grad_features, grad_weight, params[weight.size :])


def solution(mesh):
    finer = Mesh(mesh.devices.reshape(4, 8, 4, 2), ALL)
    return jax.shard_map(
        body,
        mesh=finer,
        in_specs=(
            P(ALL, None),
            P(),
            P(),
            P(ALL, None, None),
            P(ALL),
            P(ALL),
            P(ALL),
            P(ALL, None),
        ),
        out_specs=(P(ALL, None), P(ALL, None), P(), P()),
        check_vma=False,
    )
```

```python
import functools
import math

import jax
import jax.numpy as jnp
from jax import lax
from jax.experimental import pallas as pl
from jax.experimental.pallas import tpu as pltpu
from jax.sharding import Mesh
from jax.sharding import PartitionSpec as P

CAP = 2
MESH = pl.DeviceIdType.MESH
AX, AZ, AY, AC = "blk_0", "blk_1", "sub_0", "sub_1"
ALL = (AX, AZ, AY, AC)
BLK = (AX, AZ)
F32 = jnp.float32


def copy_to(src, dst, sends, recvs, at, where):
    return pltpu.make_async_remote_copy(
        src_ref=src,
        dst_ref=dst,
        send_sem=sends.at[at],
        recv_sem=recvs.at[at],
        device_id=where,
        device_id_type=MESH,
    )


def greet(places):
    barrier = pltpu.get_barrier_semaphore()
    for place in places:
        pl.semaphore_signal(barrier, inc=1, device_id=place, device_id_type=MESH)
    pl.semaphore_wait(barrier, len(places))


def visiting_order(count):
    order = [0]
    for step in range(1, count // 2 + 1):
        order.append(step)
        if count - step > count // 2:
            order.append(count - step)
    return order


def pull_kernel(sizes, first, fuse, *refs):
    nx, nz, ny = sizes
    refs = list(refs)

    def take(count):
        taken, refs[:count] = refs[:count], []
        return taken

    if first:
        ids_ref, own_ref, near_ref = take(3)
        out_ref, moved_ref, told_ref = take(3)
    else:
        asks, own_ref, near_ref, moved_ref = take(4)
        (out_ref,) = take(1)
    groups = take(nz)
    picks, relays, landing = take(3)
    zs, zr, ys, yr, cs, cr, xs, xr, ls = take(9)
    if first or fuse:
        (moved,) = take(1)
    if fuse:
        near, = take(1)
    if first:
        passing, tossed, table, asks = take(4)
        ts, tr, us, ur, js, jr, ms = take(7)
    own = own_ref.shape[0]
    half = own // 2
    x, z, y, c = (lax.axis_index(a) for a in (AX, AZ, AY, AC))
    east, west = {AX: (x + 1) % nx}, {AX: (x + nx - 1) % nx}
    up, down = {AZ: (z + 1) % nz}, {AZ: (z + nz - 1) % nz}
    fore, back = {AY: (y + 1) % ny}, {AY: (y + ny - 1) % ny}
    mate = {AC: 1 - c}

    def part(j, away, core, start=0, count=own):
        line = (y + away + ny) % ny
        return groups[j].at[pl.ds((line * 2 + core) * own + start, count)]

    def mine(j):
        return own_ref if j == 0 else part(j, 0, c)

    def along_z(j):
        if j <= nz // 2:
            return copy_to(mine(j - 1), part(j, 0, c), zs, zr, j, up)
        return copy_to(mine((j + 1) % nz), part(j, 0, c), zs, zr, j, down)

    def along_y(j, kind):
        if kind == 0:
            return copy_to(mine(j), part(j, 0, c), ys, yr, (j, 0), fore)
        if kind == 1:
            return copy_to(mine(j), part(j, 0, c), ys, yr, (j, 1), back)
        if kind == 2:
            piece = part(j, -1, c, 0, half)
            return copy_to(piece, piece, ys, yr, (j, 2), fore)
        piece = part(j, 1, c, half, half)
        return copy_to(piece, piece, ys, yr, (j, 3), back)

    def landed_y(j, kind):
        if kind == 0:
            piece = part(j, -1, c)
        elif kind == 1:
            piece = part(j, 1, c)
        elif kind == 2:
            piece = part(j, 2, c, 0, half)
        else:
            piece = part(j, 2, c, half, half)
        copy_to(piece, piece, ys, yr, (j, kind), fore).wait_recv()

    def to_mate(j, kind):
        away = (0, -1, 1, 2)[kind]
        source = mine(j) if kind == 0 else part(j, away, c)
        return copy_to(source, part(j, away, c), cs, cr, (j, kind), mate)

    def landed_mate(j, kind):
        piece = part(j, (0, -1, 1, 2)[kind], 1 - c)
        copy_to(piece, piece, cs, cr, (j, kind), mate).wait_recv()

    def far(j):
        return (z + nz - j) % nz

    def row(away):
        return (x + away + nx) % nx

    def along_x(j, kind):
        if kind == 0:
            return copy_to(picks.at[j, pl.ds(0, 4)], landing.at[x, far(j)], xs, xr, (j, 0), east)
        if kind == 1:
            return copy_to(picks.at[j, pl.ds(4, 4)], landing.at[x, far(j)], xs, xr, (j, 1), west)
        if kind == 2:
            return copy_to(picks.at[j, pl.ds(8, 2)], relays.at[j, 0], xs, xr, (j, 2), east)
        if kind == 3:
            return copy_to(picks.at[j, pl.ds(10, 2)], relays.at[j, 1], xs, xr, (j, 3), west)
        if kind == 4:
            place = landing.at[row(-1), far(j), pl.ds(0, 2)]
            return copy_to(relays.at[j, 0], place, xs, xr, (j, 4), east)
        place = landing.at[row(1), far(j), pl.ds(2, 2)]
        return copy_to(relays.at[j, 1], place, xs, xr, (j, 5), west)

    def landed_x(j, kind):
        if kind == 0:
            piece = landing.at[row(-1), far(j)]
        elif kind == 1:
            piece = landing.at[row(1), far(j)]
        elif kind in (2, 3):
            piece = relays.at[j, kind - 2]
        elif kind == 4:
            piece = landing.at[row(2), far(j), pl.ds(0, 2)]
        else:
            piece = landing.at[row(2), far(j), pl.ds(2, 2)]
        copy_to(piece, piece, xs, xr, (j, kind), east).wait_recv()

    def tiles_z(d):
        there = (z + d) % nz
        return copy_to(near_ref.at[:, there], passing.at[d], ts, tr, d, {AZ: there})

    def tiles_for(j, away):
        return near_ref.at[row(away), z] if j == 0 else passing.at[j, row(away)]

    def tiles_x(j, kind):
        if kind == 0:
            return copy_to(tiles_for(j, 1), moved.at[x, far(j)], us, ur, (j, 0), east)
        if kind == 1:
            return copy_to(tiles_for(j, -1), moved.at[x, far(j)], us, ur, (j, 1), west)
        if kind == 2:
            return copy_to(tiles_for(j, 2).at[0], tossed.at[j, 0], us, ur, (j, 2), east)
        if kind == 3:
            return copy_to(tiles_for(j, 2).at[1], tossed.at[j, 1], us, ur, (j, 3), west)
        if kind == 4:
            return copy_to(tossed.at[j, 0], moved.at[row(-1), far(j), 0], us, ur, (j, 4), east)
        return copy_to(tossed.at[j, 1], moved.at[row(1), far(j), 1], us, ur, (j, 5), west)

    def landed_tiles(j, kind):
        if kind == 0:
            piece = moved.at[row(-1), far(j)]
        elif kind == 1:
            piece = moved.at[row(1), far(j)]
        elif kind in (2, 3):
            piece = tossed.at[j, kind - 2]
        elif kind == 4:
            piece = moved.at[row(2), far(j), 0]
        else:
            piece = moved.at[row(2), far(j), 1]
        copy_to(piece, piece, us, ur, (j, kind), east).wait_recv()

    def ids_z(d):
        return copy_to(ids_ref, table.at[x, z], js, jr, d, {AZ: (z + d) % nz})

    def ids_x(d):
        return copy_to(table.at[x], table.at[x], js, jr, nz + d, {AX: (x + d) % nx})

    kept_tiles = lambda: pltpu.make_async_copy(near_ref.at[x, z], moved.at[x, z], ls.at[0])
    all_near = lambda: pltpu.make_async_copy(near_ref, near, ls.at[1])
    all_moved = lambda: pltpu.make_async_copy(moved_ref, moved, ls.at[2])
    all_asks = lambda: pltpu.make_async_copy(table, asks, ls.at[3])

    def results(j):
        return pltpu.make_async_copy(landing.at[:, far(j)], out_ref.at[:, far(j)], ls.at[4 + j])

    def moved_out(j):
        return pltpu.make_async_copy(moved.at[:, far(j)], moved_ref.at[:, far(j)], ms.at[j])

    order = visiting_order(nz)
    here = {0}

    def await_z(j):
        if j not in here:
            here.add(j)
            along_z(j).wait_recv()

    def z_step(k):
        for j, step in ((k, 1), (nz - k, -1)):
            ahead = j + step
            if k == 0:
                j, ahead = 0, (1 if step == 1 else nz - 1)
            if step == 1 and ahead > nz // 2 or step == -1 and ahead <= nz // 2:
                continue
            await_z(j)
            along_z(ahead).start()

    def tile_step(k):
        if first and k <= nz // 2:
            for d in sorted({k, nz - k}):
                tiles_z(d).start()

    def spread(j):
        await_z(j)
        along_y(j, 0).start()
        along_y(j, 1).start()
        to_mate(j, 0).start()

    def pass_on(j):
        landed_y(j, 0)
        along_y(j, 2).start()
        landed_y(j, 1)
        along_y(j, 3).start()
        to_mate(j, 1).start()
        to_mate(j, 2).start()
        landed_y(j, 2)
        landed_y(j, 3)
        to_mate(j, 3).start()

    def pick(j):
        for kind in range(4):
            landed_mate(j, kind)

        def asked(away, slot, late):
            line = row(away)
            if late:
                return asks[x, far(j), 0, (line * nz + z) * CAP + slot]
            return asks[line, z, 0, nx * nz * CAP + (x * nz + far(j)) * CAP + slot]

        def one(slot, carry):
            for late in range(2):
                place = late * CAP + slot
                picks[j, place] = groups[j][asked(1, slot, late)]
                picks[j, 4 + place] = groups[j][asked(-1, slot, late)]
                picks[j, 8 + place] = groups[j][asked(2, slot, late)]
                landing[x, far(j), place] = groups[j][asked(0, slot, late)]
            return carry

        lax.fori_loop(0, CAP, one, 0)

    def answer(j):
        for kind in (2, 3, 0, 1):
            along_x(j, kind).start()
        if first:
            if j:
                tiles_z(j).wait_recv()
                moved[x, far(j)] = passing[j, x]
            for kind in (2, 3, 0, 1):
                tiles_x(j, kind).start()

    def relay(j):
        for kind in (2, 3):
            landed_x(j, kind)
            along_x(j, kind + 2).start()
        if first:
            for kind in (2, 3):
                landed_tiles(j, kind)
                tiles_x(j, kind + 2).start()

    def finish(j):
        for kind in (0, 1, 4, 5):
            landed_x(j, kind)
            if first:
                landed_tiles(j, kind)
        if fuse:

            def one(line, carry):
                for slot in range(CAP):
                    value = landing[line, far(j), slot]
                    landing[line, far(j), slot] = product(near[line, far(j), slot], value, False)
                    value = landing[line, far(j), CAP + slot]
                    tile = moved[line, far(j), slot]
                    landing[line, far(j), CAP + slot] = product(tile, value, True)
                return carry

            lax.fori_loop(0, nx, one, 0)
        results(j).start()
        if first:
            moved_out(j).start()

    places = [east, west, up, down, fore, back, mate]
    if first:
        places += [{AX: (x + 2) % nx}] + [{AZ: (z + d) % nz} for d in range(2, nz - 1)]
    greet(places)
    if first:
        for d in range(1, nz):
            ids_z(d).start()
    z_step(0)
    spread(0)
    if first:
        kept_tiles().start()
        table[x, z] = ids_ref[...]
    elif fuse:
        all_moved().start()
    if fuse:
        all_near().start()
    groups[0][pl.ds((y * 2 + c) * own, own)] = own_ref[...]
    spread(order[1])
    z_step(1)
    if first:
        for d in range(1, nz):
            copy_to(table.at[x, far(d)], table.at[x, far(d)], js, jr, d, up).wait_recv()
        for d in range(1, nx):
            ids_x(d).start()
    for n, j in enumerate(order):
        pass_on(j)
        if n == 0:
            if first:
                kept_tiles().wait()
                for d in range(1, nx):
                    copy_to(table.at[row(-d)], table.at[row(-d)], js, jr, nz + d, east).wait_recv()
                all_asks().start()
                all_asks().wait()
            elif fuse:
                all_moved().wait()
            if fuse:
                all_near().wait()
        pick(j)
        if n + 2 < nz:
            spread(order[n + 2])
        if n + 2 < nz // 2:
            z_step(n + 2)
        if n == 2:
            for k in range(3, nz // 2 + 1):
                tile_step(k)
        elif n < 2:
            tile_step(n + 1)
        if n:
            relay(order[n - 1])
        answer(j)
        if n > 1:
            finish(order[n - 2])
    relay(order[-1])
    finish(order[-2])
    finish(order[-1])
    if first:
        told_ref[...] = table[...]
    for j in order:
        results(j).wait()
        if j:
            along_z(j).wait_send()
        for kind in range(4):
            along_y(j, kind).wait_send()
            to_mate(j, kind).wait_send()
        for kind in range(6):
            along_x(j, kind).wait_send()
        if first:
            moved_out(j).wait()
            for kind in range(6):
                tiles_x(j, kind).wait_send()
            if j:
                tiles_z(j).wait_send()
                ids_z(j).wait_send()
    if first:
        for d in range(1, nx):
            ids_x(d).wait_send()


FUSE = True


def pull(sizes, asks, value, near, moved=None):
    nx, nz, ny = sizes
    first = moved is None
    own, rows, width = value.shape
    block = (rows, width)
    dma = pltpu.SemaphoreType.DMA
    tiles = (nx, nz, CAP, rows, rows)
    values = (nx, nz, 2 * CAP, *block)
    anywhere, vmem = pl.BlockSpec(memory_space=pl.ANY), pl.BlockSpec(memory_space=pltpu.VMEM)
    smem = pl.BlockSpec(memory_space=pltpu.SMEM)
    out_shape = [jax.ShapeDtypeStruct(values, F32)]
    out_specs = [anywhere]
    in_specs = [smem, vmem, anywhere, anywhere]
    scratch = [pltpu.VMEM((ny * 2 * own, *block), F32) for _ in range(nz)] + [
        pltpu.VMEM((nz, 12, *block), F32),
        pltpu.VMEM((nz, 2, 2, *block), F32),
        pltpu.VMEM(values, F32),
        dma((nz,)),
        dma((nz,)),
        dma((nz, 4)),
        dma((nz, 4)),
        dma((nz, 4)),
        dma((nz, 4)),
        dma((nz, 6)),
        dma((nz, 6)),
        dma((4 + nz,)),
    ]
    operands = [asks, value, near, moved]
    if first or FUSE:
        scratch += [pltpu.VMEM(tiles, F32)]
    if FUSE:
        scratch += [pltpu.VMEM(tiles, F32)]
    if first:
        in_specs = [vmem, vmem, anywhere]
        operands = operands[:3]
        told = (nx, nz, *asks.shape)
        out_shape += [jax.ShapeDtypeStruct(tiles, F32), jax.ShapeDtypeStruct(told, jnp.int32)]
        out_specs += [anywhere, vmem]
        scratch += [
            pltpu.VMEM((nz, nx, CAP, rows, rows), F32),
            pltpu.VMEM((nz, 2, rows, rows), F32),
            pltpu.VMEM(told, jnp.int32),
            pltpu.SMEM(told, jnp.int32),
            dma((nz,)),
            dma((nz,)),
            dma((nz, 6)),
            dma((nz, 6)),
            dma((nz + nx,)),
            dma((nz + nx,)),
            dma((nz,)),
        ]
    return pl.pallas_call(
        functools.partial(pull_kernel, sizes, first, FUSE),
        out_shape=out_shape,
        in_specs=in_specs,
        out_specs=out_specs,
        scratch_shapes=scratch,
        compiler_params=pltpu.CompilerParams(
            collective_id=0 if first else 2,
            has_side_effects=True,
            vmem_limit_bytes=58 * 2**20,
        ),
        cost_estimate=pl.CostEstimate(
            flops=20_000_000_000, bytes_accessed=17_000_000, transcendentals=0
        ),
        name="pull_first" if first else "pull_again",
    )(*operands)


def scatter_kernel(ny, sums, out_ref, mated, total, early, late, cs, cr, ys, yr):
    own = out_ref.shape[0]
    half = own // 2
    y, c = lax.axis_index(AY), lax.axis_index(AC)
    fore, back, mate = {AY: (y + 1) % ny}, {AY: (y + ny - 1) % ny}, {AC: 1 - c}

    def at(away, core):
        return pl.ds((((y + away) % ny) * 2 + core) * own, own)

    def over(k):
        return copy_to(sums.at[at(k, 1 - c)], mated.at[k], cs, cr, k, mate)

    early_fore = copy_to(total.at[2, pl.ds(0, half)], early.at[0], ys, yr, 0, fore)
    early_back = copy_to(total.at[2, pl.ds(half, half)], early.at[1], ys, yr, 1, back)
    late_fore = copy_to(total.at[1], late.at[0], ys, yr, 2, fore)
    late_back = copy_to(total.at[3], late.at[1], ys, yr, 3, back)
    greet((fore, back, mate))
    for k in (2, 1, 3, 0):
        over(k).start()
    for k in (2, 1, 3, 0):
        over(k).wait_recv()
        total[k] = sums[at(k, c)] + mated[k]
        if k == 1:
            early_fore.start()
            early_back.start()
    early_fore.wait_recv()
    total[1, pl.ds(0, half)] = total[1, pl.ds(0, half)] + early[0]
    early_back.wait_recv()
    total[3, pl.ds(half, half)] = total[3, pl.ds(half, half)] + early[1]
    late_fore.start()
    late_back.start()
    late_fore.wait_recv()
    late_back.wait_recv()
    out_ref[...] = total[0] + late[0] + late[1]
    for k in range(4):
        over(k).wait_send()
    for copy in (early_fore, early_back, late_fore, late_back):
        copy.wait_send()


def scatter(ny, sums):
    count, rows, width = sums.shape
    own = count // (2 * ny)
    dma = pltpu.SemaphoreType.DMA
    piece = (own, rows, width)
    return pl.pallas_call(
        functools.partial(scatter_kernel, ny),
        out_shape=jax.ShapeDtypeStruct(piece, F32),
        in_specs=[pl.BlockSpec(memory_space=pltpu.VMEM)],
        out_specs=pl.BlockSpec(memory_space=pltpu.VMEM),
        scratch_shapes=[
            pltpu.VMEM((4, *piece), F32),
            pltpu.VMEM((4, *piece), F32),
            pltpu.VMEM((2, own // 2, rows, width), F32),
            pltpu.VMEM((2, *piece), F32),
            dma((4,)),
            dma((4,)),
            dma((4,)),
            dma((4,)),
        ],
        compiler_params=pltpu.CompilerParams(
            collective_id=1, has_side_effects=True, vmem_limit_bytes=16 * 2**20
        ),
        cost_estimate=pl.CostEstimate(
            flops=2_000_000_000, bytes_accessed=2_000_000, transcendentals=0
        ),
        name="scatter",
    )(sums)


def halves(value):
    high = value.astype(jnp.bfloat16)
    return high, (value - high.astype(F32)).astype(jnp.bfloat16)


def product(tile, value, flipped):
    dims = (((0 if flipped else 1,), (0,)), ((), ()))
    tile_high, tile_low = halves(tile)
    high, low = halves(value)

    def dot(a, b):
        return lax.dot_general(a, b, dims, preferred_element_type=F32)

    return dot(tile_high, high) + (dot(tile_high, low) + dot(tile_low, high))


def add_kernel(step, group, told, products, sums):
    first = pl.program_id(0) * step
    count = pl.num_programs(0) * step * CAP
    me = group[0]

    @pl.when(first == 0)
    def _():
        sums[...] = jnp.zeros_like(sums)

    for g in range(step):
        for slot in range(2 * CAP):
            if slot < CAP:
                at = me * (4 * count) + (first + g) * CAP + slot
                alive, target = told[at + 2 * count], told[at]
            else:
                at = (first + g) * (4 * count) + me * CAP + slot - CAP
                alive, target = told[at + 2 * count], told[at + count]

            @pl.when(alive > 0)
            def _(target=target, g=g, slot=slot):
                sums[target] += products[g, slot]


def add(group_size, group, told, products):
    count, slots, rows, width = products.shape
    step = 4
    return pl.pallas_call(
        functools.partial(add_kernel, step),
        out_shape=jax.ShapeDtypeStruct((group_size, rows, width), F32),
        grid_spec=pltpu.PrefetchScalarGridSpec(
            num_scalar_prefetch=2,
            grid=(count // step,),
            in_specs=[pl.BlockSpec((step, slots, rows, width), lambda n, *_: (n, 0, 0, 0))],
            out_specs=pl.BlockSpec((group_size, rows, width), lambda n, *_: (0, 0, 0)),
        ),
        compiler_params=pltpu.CompilerParams(vmem_limit_bytes=58 * 2**20),
        cost_estimate=pl.CostEstimate(
            flops=count * slots * rows * width, bytes_accessed=11_000_000, transcendentals=0
        ),
        name="add",
    )(group, told, products)


def exchanged(value, axis):
    return lax.all_to_all(value, axis, 0, 0, tiled=True)


def far_sum(pieces, axis):
    return exchanged(pieces, axis).sum(axis=0)


def for_each(value, axis):
    peers = lax.axis_size(axis)
    return exchanged(jnp.broadcast_to(value[None], (peers, *value.shape)), axis)


def param_sum(vector):
    blocks, subs = lax.axis_size(BLK), lax.axis_size((AY, AC))
    spare = -vector.shape[0] % (blocks * subs)
    padded = jnp.concatenate([vector, jnp.zeros((spare,), F32)]).reshape(blocks, subs, -1)
    near = far_sum(padded.swapaxes(0, 1), (AY, AC))
    done = far_sum(near, BLK)
    line = for_each(done, BLK)
    whole = for_each(line, (AY, AC))
    return whole.swapaxes(0, 1).reshape(-1)[: vector.shape[0]]


def body(features, weight, bias, adj_tiles, tile_rows, tile_cols, tile_counts, cotangent):
    nx, nz, ny = (lax.axis_size(a) for a in (AX, AZ, AY))
    sizes = (nx, nz, ny)
    blocks = nx * nz
    rows, width = adj_tiles.shape[1], features.shape[1]
    own = features.shape[0] // rows
    group_size = own * ny * 2
    group = lax.axis_index(BLK)
    scale = 1.0 / math.sqrt(features.shape[0] * blocks * ny * 2)
    slots = jnp.arange(blocks * CAP, dtype=jnp.int32)
    alive = (slots % CAP < tile_counts[slots // CAP]).astype(jnp.int32)
    row_local = tile_rows - group * group_size
    col_local = tile_cols - slots // CAP * group_size
    ids = jnp.concatenate([row_local, col_local, alive, alive]).reshape(2, -1)
    near = adj_tiles.reshape(nx, nz, CAP, rows, rows)

    def aggregate(value, asks, moved=None):
        pulled = pull(sizes, asks, value.reshape(own, rows, width), near, moved)
        if moved is None:
            products, moved, asks = pulled
        else:
            (products,) = pulled
        products = products.reshape(blocks, 2 * CAP, rows, width)
        me = group.astype(jnp.int32).reshape(1)
        sums = add(group_size, me, asks.reshape(-1), products)
        return scatter(ny, sums).reshape(value.shape), asks, moved

    dot = functools.partial(jnp.dot, precision=lax.Precision.HIGHEST)
    spread, asks, moved = aggregate(features, ids)
    pre = dot(spread, weight) + bias
    sigma = jax.nn.sigmoid(pre)
    activation = pre * sigma
    grad_pre = cotangent * sigma * (1.0 + pre * (1.0 - sigma))
    vector = jnp.concatenate(
        [(dot(spread.T, grad_pre) * scale).reshape(-1), jnp.sum(grad_pre, axis=0) * scale]
    )
    params = param_sum(vector)
    grad_mixed = aggregate(grad_pre, asks, moved)[0]
    grad_features = dot(grad_mixed, weight.T)
    grad_weight = params[: weight.size].reshape(weight.shape)
    return (activation, grad_features, grad_weight, params[weight.size :])


def solution(mesh):
    finer = Mesh(mesh.devices.reshape(4, 8, 4, 2), ALL)
    return jax.shard_map(
        body,
        mesh=finer,
        in_specs=(
            P(ALL, None),
            P(),
            P(),
            P(ALL, None, None),
            P(ALL),
            P(ALL),
            P(ALL),
            P(ALL, None),
        ),
        out_specs=(P(ALL, None), P(ALL, None), P(), P()),
        check_vma=False,
    )
```

```python
import functools
import math

import jax
import jax.numpy as jnp
from jax import lax
from jax.experimental import pallas as pl
from jax.experimental.pallas import tpu as pltpu
from jax.sharding import Mesh
from jax.sharding import PartitionSpec as P

CAP = 2
MESH = pl.DeviceIdType.MESH
AX, AZ, AY, AC = "blk_0", "blk_1", "sub_0", "sub_1"
ALL = (AX, AZ, AY, AC)
BLK = (AX, AZ)
F32 = jnp.float32


def copy_to(src, dst, sends, recvs, at, where):
    return pltpu.make_async_remote_copy(
        src_ref=src,
        dst_ref=dst,
        send_sem=sends.at[at],
        recv_sem=recvs.at[at],
        device_id=where,
        device_id_type=MESH,
    )


def greet(places):
    barrier = pltpu.get_barrier_semaphore()
    for place in places:
        pl.semaphore_signal(barrier, inc=1, device_id=place, device_id_type=MESH)
    pl.semaphore_wait(barrier, len(places))


def visiting_order(count):
    order = [0]
    for step in range(1, count // 2 + 1):
        order.append(step)
        if count - step > count // 2:
            order.append(count - step)
    return order


def pull_kernel(sizes, first, fuse, *refs):
    nx, nz, ny = sizes
    refs = list(refs)

    def take(count):
        taken, refs[:count] = refs[:count], []
        return taken

    if first:
        ids_ref, own_ref, near_ref = take(3)
        out_ref, moved_ref, told_ref = take(3)
    else:
        asks, own_ref, near_ref, moved_ref, terms_ref = take(5)
        out_ref, whole_ref = take(2)
    groups = take(nz)
    picks, relays, landing = take(3)
    zs, zr, ys, yr, cs, cr, xs, xr, ls = take(9)
    if first or fuse:
        (moved,) = take(1)
    if fuse:
        near, = take(1)
    if first:
        passing, tossed, table, asks = take(4)
        ts, tr, us, ur, js, jr, ms = take(7)
    else:
        cut, stack, pile, joined, ps, pr = take(6)
    own = own_ref.shape[0]
    half = own // 2
    x, z, y, c = (lax.axis_index(a) for a in (AX, AZ, AY, AC))
    east, west = {AX: (x + 1) % nx}, {AX: (x + nx - 1) % nx}
    up, down = {AZ: (z + 1) % nz}, {AZ: (z + nz - 1) % nz}
    fore, back = {AY: (y + 1) % ny}, {AY: (y + ny - 1) % ny}
    mate = {AC: 1 - c}

    def part(j, away, core, start=0, count=own):
        line = (y + away + ny) % ny
        return groups[j].at[pl.ds((line * 2 + core) * own + start, count)]

    def mine(j):
        return own_ref if j == 0 else part(j, 0, c)

    def along_z(j):
        if j <= nz // 2:
            return copy_to(mine(j - 1), part(j, 0, c), zs, zr, j, up)
        return copy_to(mine((j + 1) % nz), part(j, 0, c), zs, zr, j, down)

    def along_y(j, kind):
        if kind == 2:
            piece = part(j, -1, c, 0, half)
            return copy_to(piece, piece, ys, yr, (j, 2), fore)
        if kind == 3:
            piece = part(j, 1, c, half, half)
            return copy_to(piece, piece, ys, yr, (j, 3), back)
        start = 0 if kind in (0, 5) else half
        source = own_ref.at[pl.ds(start, half)] if j == 0 else part(j, 0, c, start, half)
        where = fore if kind in (0, 4) else back
        return copy_to(source, part(j, 0, c, start, half), ys, yr, (j, kind), where)

    def landed_y(j, kind):
        away = (-1, 1, 2, 2, -1, 1)[kind]
        piece = part(j, away, c, 0 if kind in (0, 2, 5) else half, half)
        copy_to(piece, piece, ys, yr, (j, kind), fore).wait_recv()

    def to_mate(j, kind):
        away = (0, -1, 1, 2)[kind]
        source = mine(j) if kind == 0 else part(j, away, c)
        return copy_to(source, part(j, away, c), cs, cr, (j, kind), mate)

    def landed_mate(j, kind):
        piece = part(j, (0, -1, 1, 2)[kind], 1 - c)
        copy_to(piece, piece, cs, cr, (j, kind), mate).wait_recv()

    def far(j):
        return (z + nz - j) % nz

    def row(away):
        return (x + away + nx) % nx

    def along_x(j, kind):
        if kind == 0:
            return copy_to(picks.at[j, pl.ds(0, 4)], landing.at[x, far(j)], xs, xr, (j, 0), east)
        if kind == 1:
            return copy_to(picks.at[j, pl.ds(4, 4)], landing.at[x, far(j)], xs, xr, (j, 1), west)
        if kind == 2:
            return copy_to(picks.at[j, pl.ds(8, 2)], relays.at[j, 0], xs, xr, (j, 2), east)
        if kind == 3:
            return copy_to(picks.at[j, pl.ds(10, 2)], relays.at[j, 1], xs, xr, (j, 3), west)
        if kind == 4:
            place = landing.at[row(-1), far(j), pl.ds(0, 2)]
            return copy_to(relays.at[j, 0], place, xs, xr, (j, 4), east)
        place = landing.at[row(1), far(j), pl.ds(2, 2)]
        return copy_to(relays.at[j, 1], place, xs, xr, (j, 5), west)

    def landed_x(j, kind):
        if kind == 0:
            piece = landing.at[row(-1), far(j)]
        elif kind == 1:
            piece = landing.at[row(1), far(j)]
        elif kind in (2, 3):
            piece = relays.at[j, kind - 2]
        elif kind == 4:
            piece = landing.at[row(2), far(j), pl.ds(0, 2)]
        else:
            piece = landing.at[row(2), far(j), pl.ds(2, 2)]
        copy_to(piece, piece, xs, xr, (j, kind), east).wait_recv()

    def tiles_z(d):
        there = (z + d) % nz
        return copy_to(near_ref.at[:, there], passing.at[d], ts, tr, d, {AZ: there})

    def tiles_for(j, away):
        return near_ref.at[row(away), z] if j == 0 else passing.at[j, row(away)]

    def tiles_x(j, kind):
        if kind == 0:
            return copy_to(tiles_for(j, 1), moved.at[x, far(j)], us, ur, (j, 0), east)
        if kind == 1:
            return copy_to(tiles_for(j, -1), moved.at[x, far(j)], us, ur, (j, 1), west)
        if kind == 2:
            return copy_to(tiles_for(j, 2).at[0], tossed.at[j, 0], us, ur, (j, 2), east)
        if kind == 3:
            return copy_to(tiles_for(j, 2).at[1], tossed.at[j, 1], us, ur, (j, 3), west)
        if kind == 4:
            return copy_to(tossed.at[j, 0], moved.at[row(-1), far(j), 0], us, ur, (j, 4), east)
        return copy_to(tossed.at[j, 1], moved.at[row(1), far(j), 1], us, ur, (j, 5), west)

    def landed_tiles(j, kind):
        if kind == 0:
            piece = moved.at[row(-1), far(j)]
        elif kind == 1:
            piece = moved.at[row(1), far(j)]
        elif kind in (2, 3):
            piece = tossed.at[j, kind - 2]
        elif kind == 4:
            piece = moved.at[row(2), far(j), 0]
        else:
            piece = moved.at[row(2), far(j), 1]
        copy_to(piece, piece, us, ur, (j, kind), east).wait_recv()

    def ids_z(d):
        return copy_to(ids_ref, table.at[x, z], js, jr, d, {AZ: (z + d) % nz})

    def ids_x(d):
        return copy_to(table.at[x], table.at[x], js, jr, nz + d, {AX: (x + d) % nx})

    kept_tiles = lambda: pltpu.make_async_copy(near_ref.at[x, z], moved.at[x, z], ls.at[0])
    all_near = lambda: pltpu.make_async_copy(near_ref, near, ls.at[1])
    all_moved = lambda: pltpu.make_async_copy(moved_ref, moved, ls.at[2])
    all_asks = lambda: pltpu.make_async_copy(table, asks, ls.at[3])

    def results(j):
        return pltpu.make_async_copy(landing.at[:, far(j)], out_ref.at[:, far(j)], ls.at[4 + j])

    def moved_out(j):
        return pltpu.make_async_copy(moved.at[:, far(j)], moved_ref.at[:, far(j)], ms.at[j])

    nsub = 2 * ny
    sub = y * 2 + c

    def sub_place(d):
        there = (sub + d) % nsub
        return {AY: there // 2, AC: there % 2}

    def term(stage, d):
        if stage == 0:
            source = terms_ref.at[(sub + d) % nsub]
            return copy_to(source, cut.at[sub], ps, pr, d, sub_place(d))
        if stage == 1:
            return copy_to(stack.at[z], stack.at[z], ps, pr, nsub + d, {AZ: (z + d) % nz})
        at = nsub + nz + d
        if stage == 2:
            return copy_to(pile.at[x], pile.at[x], ps, pr, at, {AX: (x + d) % nx})
        return copy_to(joined.at[sub], joined.at[sub], ps, pr, at + nx, sub_place(d))

    def term_landed(stage, d):
        back_by = lambda me, count: (me + count - d) % count
        if stage == 0:
            piece, at = cut.at[back_by(sub, nsub)], d
        elif stage == 1:
            piece, at = stack.at[back_by(z, nz)], nsub + d
        elif stage == 2:
            piece, at = pile.at[back_by(x, nx)], nsub + nz + d
        else:
            piece, at = joined.at[back_by(sub, nsub)], nsub + nz + nx + d
        copy_to(piece, piece, ps, pr, at, mate).wait_recv()

    def terms_in(stage):
        return range(1, (nsub, nz, nx, nsub)[stage])

    def send_terms(stage):
        for d in terms_in(stage):
            term(stage, d).start()

    def sum_terms(stage):
        for d in terms_in(stage):
            term_landed(stage, d)
        source, count = ((cut, nsub), (stack, nz), (pile, nx))[stage]
        total = source[0]
        for k in range(1, count):
            total = total + source[k]
        if stage == 0:
            stack[z] = total
        elif stage == 1:
            pile[x] = total
        else:
            joined[sub] = total

    order = visiting_order(nz)
    here = {0}

    def await_z(j):
        if j not in here:
            here.add(j)
            along_z(j).wait_recv()

    def z_step(k):
        for j, step in ((k, 1), (nz - k, -1)):
            ahead = j + step
            if k == 0:
                j, ahead = 0, (1 if step == 1 else nz - 1)
            if step == 1 and ahead > nz // 2 or step == -1 and ahead <= nz // 2:
                continue
            await_z(j)
            along_z(ahead).start()

    def tile_step(k):
        if first and k <= nz // 2:
            for d in sorted({k, nz - k}):
                tiles_z(d).start()

    def spread(j):
        await_z(j)
        for kind in (0, 1, 4, 5):
            along_y(j, kind).start()
        to_mate(j, 0).start()

    def pass_on(j):
        landed_y(j, 0)
        along_y(j, 2).start()
        landed_y(j, 1)
        along_y(j, 3).start()
        landed_y(j, 4)
        to_mate(j, 1).start()
        landed_y(j, 5)
        to_mate(j, 2).start()
        landed_y(j, 2)
        landed_y(j, 3)
        to_mate(j, 3).start()

    def pick(j):
        for kind in range(4):
            landed_mate(j, kind)

        def asked(away, slot, late):
            line = row(away)
            if late:
                return asks[x, far(j), 0, (line * nz + z) * CAP + slot]
            return asks[line, z, 0, nx * nz * CAP + (x * nz + far(j)) * CAP + slot]

        def one(slot, carry):
            for late in range(2):
                place = late * CAP + slot
                picks[j, place] = groups[j][asked(1, slot, late)]
                picks[j, 4 + place] = groups[j][asked(-1, slot, late)]
                picks[j, 8 + place] = groups[j][asked(2, slot, late)]
                landing[x, far(j), place] = groups[j][asked(0, slot, late)]
            return carry

        lax.fori_loop(0, CAP, one, 0)

    def answer(j):
        for kind in (2, 3, 0, 1):
            along_x(j, kind).start()
        if first and j:
            tiles_z(j).wait_recv()
            moved[x, far(j)] = passing[j, x]
            for kind in (2, 3, 0, 1):
                tiles_x(j, kind).start()

    def relay(j):
        for kind in (2, 3):
            landed_x(j, kind)
            along_x(j, kind + 2).start()
        if first:
            for kind in (2, 3):
                landed_tiles(j, kind)
                tiles_x(j, kind + 2).start()

    def finish(j):
        for kind in (0, 1, 4, 5):
            landed_x(j, kind)
            if first:
                landed_tiles(j, kind)
        if fuse:

            def one(line, carry):
                for slot in range(CAP):
                    value = landing[line, far(j), slot]
                    landing[line, far(j), slot] = product(near[line, far(j), slot], value, False)
                    value = landing[line, far(j), CAP + slot]
                    tile = moved[line, far(j), slot]
                    landing[line, far(j), CAP + slot] = product(tile, value, True)
                return carry

            lax.fori_loop(0, nx, one, 0)
        results(j).start()
        if first:
            moved_out(j).start()

    places = [east, west, up, down, fore, back, mate]
    if first:
        places += [{AX: (x + 2) % nx}] + [{AZ: (z + d) % nz} for d in range(2, nz - 1)]
    else:
        places = [{AX: (x + d) % nx} for d in range(1, nx)]
        places += [{AZ: (z + d) % nz} for d in range(1, nz)]
        places += [sub_place(d) for d in range(1, nsub)]
    greet(places)
    if not first:
        send_terms(0)
    if first:
        for d in range(1, nz):
            ids_z(d).start()
        for kind in (2, 3, 0, 1):
            tiles_x(0, kind).start()
    z_step(0)
    spread(0)
    if first:
        kept_tiles().start()
        table[x, z] = ids_ref[...]
    elif fuse:
        all_moved().start()
        cut[sub] = terms_ref[sub]
    if fuse:
        all_near().start()
    groups[0][pl.ds((y * 2 + c) * own, own)] = own_ref[...]
    spread(order[1])
    z_step(1)
    if first:
        for d in range(1, nz):
            copy_to(table.at[x, far(d)], table.at[x, far(d)], js, jr, d, up).wait_recv()
        for d in range(1, nx):
            ids_x(d).start()
    stages = (1, 3, 5)
    for n, j in enumerate(order):
        pass_on(j)
        if n == 0:
            if first:
                kept_tiles().wait()
                for d in range(1, nx):
                    copy_to(table.at[row(-d)], table.at[row(-d)], js, jr, nz + d, east).wait_recv()
                all_asks().start()
                all_asks().wait()
            elif fuse:
                all_moved().wait()
            if fuse:
                all_near().wait()
        pick(j)
        if not first and n in stages:
            sum_terms(stages.index(n))
        if n + 2 < nz:
            spread(order[n + 2])
        if n + 2 < nz // 2:
            z_step(n + 2)
        if n == 2:
            for k in range(3, nz // 2 + 1):
                tile_step(k)
        elif n < 2:
            tile_step(n + 1)
        if n:
            relay(order[n - 1])
        if not first and n in stages:
            send_terms(stages.index(n) + 1)
        answer(j)
        if n > 1:
            finish(order[n - 2])
    relay(order[-1])
    finish(order[-2])
    finish(order[-1])
    if first:
        told_ref[...] = table[...]
    else:
        for d in terms_in(3):
            term_landed(3, d)
        whole_ref[...] = joined[...]
        for stage in range(4):
            for d in terms_in(stage):
                term(stage, d).wait_send()
    for j in order:
        results(j).wait()
        if j:
            along_z(j).wait_send()
        for kind in range(4):
            to_mate(j, kind).wait_send()
        for kind in range(6):
            along_y(j, kind).wait_send()
            along_x(j, kind).wait_send()
        if first:
            moved_out(j).wait()
            for kind in range(6):
                tiles_x(j, kind).wait_send()
            if j:
                tiles_z(j).wait_send()
                ids_z(j).wait_send()
    if first:
        for d in range(1, nx):
            ids_x(d).wait_send()


FUSE = True


def pull(sizes, asks, value, near, moved=None, terms=None):
    nx, nz, ny = sizes
    first = moved is None
    own, rows, width = value.shape
    block = (rows, width)
    dma = pltpu.SemaphoreType.DMA
    tiles = (nx, nz, CAP, rows, rows)
    values = (nx, nz, 2 * CAP, *block)
    anywhere, vmem = pl.BlockSpec(memory_space=pl.ANY), pl.BlockSpec(memory_space=pltpu.VMEM)
    smem = pl.BlockSpec(memory_space=pltpu.SMEM)
    out_shape = [jax.ShapeDtypeStruct(values, F32)]
    out_specs = [anywhere]
    in_specs = [smem, vmem, anywhere, anywhere, vmem]
    scratch = [pltpu.VMEM((ny * 2 * own, *block), F32) for _ in range(nz)] + [
        pltpu.VMEM((nz, 12, *block), F32),
        pltpu.VMEM((nz, 2, 2, *block), F32),
        pltpu.VMEM(values, F32),
        dma((nz,)),
        dma((nz,)),
        dma((nz, 6)),
        dma((nz, 6)),
        dma((nz, 4)),
        dma((nz, 4)),
        dma((nz, 6)),
        dma((nz, 6)),
        dma((4 + nz,)),
    ]
    operands = [asks, value, near, moved, terms]
    if first or FUSE:
        scratch += [pltpu.VMEM(tiles, F32)]
    if FUSE:
        scratch += [pltpu.VMEM(tiles, F32)]
    if first:
        in_specs = [vmem, vmem, anywhere]
        operands = operands[:3]
        told = (nx, nz, *asks.shape)
        out_shape += [jax.ShapeDtypeStruct(tiles, F32), jax.ShapeDtypeStruct(told, jnp.int32)]
        out_specs += [anywhere, vmem]
        scratch += [
            pltpu.VMEM((nz, nx, CAP, rows, rows), F32),
            pltpu.VMEM((nz, 2, rows, rows), F32),
            pltpu.VMEM(told, jnp.int32),
            pltpu.SMEM(told, jnp.int32),
            dma((nz,)),
            dma((nz,)),
            dma((nz, 6)),
            dma((nz, 6)),
            dma((nz + nx,)),
            dma((nz + nx,)),
            dma((nz,)),
        ]
    else:
        out_shape += [jax.ShapeDtypeStruct(terms.shape, F32)]
        out_specs += [vmem]
        scratch += [
            pltpu.VMEM(terms.shape, F32),
            pltpu.VMEM((nz, *terms.shape[1:]), F32),
            pltpu.VMEM((nx, *terms.shape[1:]), F32),
            pltpu.VMEM(terms.shape, F32),
            dma((4 * ny + nz + nx,)),
            dma((4 * ny + nz + nx,)),
        ]
    return pl.pallas_call(
        functools.partial(pull_kernel, sizes, first, FUSE),
        out_shape=out_shape,
        in_specs=in_specs,
        out_specs=out_specs,
        scratch_shapes=scratch,
        compiler_params=pltpu.CompilerParams(
            collective_id=0 if first else 2,
            has_side_effects=True,
            vmem_limit_bytes=58 * 2**20,
        ),
        cost_estimate=pl.CostEstimate(
            flops=20_000_000_000, bytes_accessed=17_000_000, transcendentals=0
        ),
        name="pull_first" if first else "pull_again",
    )(*operands)


def scatter_kernel(ny, sums, out_ref, mated, total, early, late, cs, cr, ys, yr):
    own = out_ref.shape[0]
    half = own // 2
    y, c = lax.axis_index(AY), lax.axis_index(AC)
    fore, back, mate = {AY: (y + 1) % ny}, {AY: (y + ny - 1) % ny}, {AC: 1 - c}

    def at(away, core):
        return pl.ds((((y + away) % ny) * 2 + core) * own, own)

    def over(k):
        return copy_to(sums.at[at(k, 1 - c)], mated.at[k], cs, cr, k, mate)

    early_fore = copy_to(total.at[2, pl.ds(0, half)], early.at[0], ys, yr, 0, fore)
    early_back = copy_to(total.at[2, pl.ds(half, half)], early.at[1], ys, yr, 1, back)
    late_fore = copy_to(total.at[1], late.at[0], ys, yr, 2, fore)
    late_back = copy_to(total.at[3], late.at[1], ys, yr, 3, back)
    greet((fore, back, mate))
    for k in (2, 1, 3, 0):
        over(k).start()
    for k in (2, 1, 3, 0):
        over(k).wait_recv()
        total[k] = sums[at(k, c)] + mated[k]
        if k == 1:
            early_fore.start()
            early_back.start()
    early_fore.wait_recv()
    total[1, pl.ds(0, half)] = total[1, pl.ds(0, half)] + early[0]
    early_back.wait_recv()
    total[3, pl.ds(half, half)] = total[3, pl.ds(half, half)] + early[1]
    late_fore.start()
    late_back.start()
    late_fore.wait_recv()
    late_back.wait_recv()
    out_ref[...] = total[0] + late[0] + late[1]
    for k in range(4):
        over(k).wait_send()
    for copy in (early_fore, early_back, late_fore, late_back):
        copy.wait_send()


def scatter(ny, sums):
    count, rows, width = sums.shape
    own = count // (2 * ny)
    dma = pltpu.SemaphoreType.DMA
    piece = (own, rows, width)
    return pl.pallas_call(
        functools.partial(scatter_kernel, ny),
        out_shape=jax.ShapeDtypeStruct(piece, F32),
        in_specs=[pl.BlockSpec(memory_space=pltpu.VMEM)],
        out_specs=pl.BlockSpec(memory_space=pltpu.VMEM),
        scratch_shapes=[
            pltpu.VMEM((4, *piece), F32),
            pltpu.VMEM((4, *piece), F32),
            pltpu.VMEM((2, own // 2, rows, width), F32),
            pltpu.VMEM((2, *piece), F32),
            dma((4,)),
            dma((4,)),
            dma((4,)),
            dma((4,)),
        ],
        compiler_params=pltpu.CompilerParams(
            collective_id=1, has_side_effects=True, vmem_limit_bytes=16 * 2**20
        ),
        cost_estimate=pl.CostEstimate(
            flops=2_000_000_000, bytes_accessed=2_000_000, transcendentals=0
        ),
        name="scatter",
    )(sums)


def halves(value):
    high = value.astype(jnp.bfloat16)
    return high, (value - high.astype(F32)).astype(jnp.bfloat16)


def product(tile, value, flipped):
    dims = (((0 if flipped else 1,), (0,)), ((), ()))
    tile_high, tile_low = halves(tile)
    high, low = halves(value)

    def dot(a, b):
        return lax.dot_general(a, b, dims, preferred_element_type=F32)

    return dot(tile_high, high) + (dot(tile_high, low) + dot(tile_low, high))


def add_kernel(step, group, told, products, sums):
    first = pl.program_id(0) * step
    count = pl.num_programs(0) * step * CAP
    me = group[0]

    @pl.when(first == 0)
    def _():
        sums[...] = jnp.zeros_like(sums)

    for g in range(step):
        for slot in range(2 * CAP):
            if slot < CAP:
                at = me * (4 * count) + (first + g) * CAP + slot
                alive, target = told[at + 2 * count], told[at]
            else:
                at = (first + g) * (4 * count) + me * CAP + slot - CAP
                alive, target = told[at + 2 * count], told[at + count]

            @pl.when(alive > 0)
            def _(target=target, g=g, slot=slot):
                sums[target] += products[g, slot]


def add(group_size, group, told, products):
    count, slots, rows, width = products.shape
    step = 4
    return pl.pallas_call(
        functools.partial(add_kernel, step),
        out_shape=jax.ShapeDtypeStruct((group_size, rows, width), F32),
        grid_spec=pltpu.PrefetchScalarGridSpec(
            num_scalar_prefetch=2,
            grid=(count // step,),
            in_specs=[pl.BlockSpec((step, slots, rows, width), lambda n, *_: (n, 0, 0, 0))],
            out_specs=pl.BlockSpec((group_size, rows, width), lambda n, *_: (0, 0, 0)),
        ),
        compiler_params=pltpu.CompilerParams(vmem_limit_bytes=58 * 2**20),
        cost_estimate=pl.CostEstimate(
            flops=count * slots * rows * width, bytes_accessed=11_000_000, transcendentals=0
        ),
        name="add",
    )(group, told, products)


def body(features, weight, bias, adj_tiles, tile_rows, tile_cols, tile_counts, cotangent):
    nx, nz, ny = (lax.axis_size(a) for a in (AX, AZ, AY))
    sizes = (nx, nz, ny)
    blocks = nx * nz
    rows, width = adj_tiles.shape[1], features.shape[1]
    own = features.shape[0] // rows
    group_size = own * ny * 2
    group = lax.axis_index(BLK)
    scale = 1.0 / math.sqrt(features.shape[0] * blocks * ny * 2)
    slots = jnp.arange(blocks * CAP, dtype=jnp.int32)
    alive = (slots % CAP < tile_counts[slots // CAP]).astype(jnp.int32)
    row_local = tile_rows - group * group_size
    col_local = tile_cols - slots // CAP * group_size
    ids = jnp.concatenate([row_local, col_local, alive, alive]).reshape(2, -1)
    near = adj_tiles.reshape(nx, nz, CAP, rows, rows)

    def collect(products, asks, shape):
        me = group.astype(jnp.int32).reshape(1)
        products = products.reshape(blocks, 2 * CAP, rows, width)
        return scatter(ny, add(group_size, me, asks.reshape(-1), products)).reshape(shape)

    dot = functools.partial(jnp.dot, precision=lax.Precision.HIGHEST)
    cut = (own, rows, width)
    products, moved, asks = pull(sizes, ids, features.reshape(cut), near)
    spread = collect(products, asks, features.shape)
    pre = dot(spread, weight) + bias
    sigma = jax.nn.sigmoid(pre)
    activation = pre * sigma
    grad_pre = cotangent * sigma * (1.0 + pre * (1.0 - sigma))
    pieces = 2 * ny
    spare = -(weight.shape[0] + 1) % (8 * pieces)
    terms = jnp.concatenate(
        [
            dot(spread.T, grad_pre) * scale,
            jnp.sum(grad_pre, axis=0)[None] * scale,
            jnp.zeros((spare, width), F32),
        ]
    ).reshape(pieces, -1, width)
    products, params = pull(sizes, asks, grad_pre.reshape(cut), near, moved, terms)
    grad_mixed = collect(products, asks, features.shape)
    grad_features = dot(grad_mixed, weight.T)
    params = params.reshape(-1, width)
    return (activation, grad_features, params[: weight.shape[0]], params[weight.shape[0]])


def solution(mesh):
    finer = Mesh(mesh.devices.reshape(4, 8, 4, 2), ALL)
    return jax.shard_map(
        body,
        mesh=finer,
        in_specs=(
            P(ALL, None),
            P(),
            P(),
            P(ALL, None, None),
            P(ALL),
            P(ALL),
            P(ALL),
            P(ALL, None),
        ),
        out_specs=(P(ALL, None), P(ALL, None), P(), P()),
        check_vma=False,
    )
```

```python
import functools
import math

import jax
import jax.numpy as jnp
from jax import lax
from jax.experimental import pallas as pl
from jax.experimental.pallas import tpu as pltpu
from jax.sharding import Mesh
from jax.sharding import PartitionSpec as P

CAP = 2
MESH = pl.DeviceIdType.MESH
AX, AZ, AY, AC = "blk_0", "blk_1", "sub_0", "sub_1"
ALL = (AX, AZ, AY, AC)
BLK = (AX, AZ)
F32 = jnp.float32


def copy_to(src, dst, sends, recvs, at, where):
    return pltpu.make_async_remote_copy(
        src_ref=src,
        dst_ref=dst,
        send_sem=sends.at[at],
        recv_sem=recvs.at[at],
        device_id=where,
        device_id_type=MESH,
    )


def greet(places):
    barrier = pltpu.get_barrier_semaphore()
    for place in places:
        pl.semaphore_signal(barrier, inc=1, device_id=place, device_id_type=MESH)
    pl.semaphore_wait(barrier, len(places))


def visiting_order(count):
    order = [0]
    for step in range(1, count // 2 + 1):
        order.append(step)
        if count - step > count // 2:
            order.append(count - step)
    return order


def pull_kernel(sizes, first, fuse, *refs):
    nx, nz, ny = sizes
    refs = list(refs)

    def take(count):
        taken, refs[:count] = refs[:count], []
        return taken

    if first:
        ids_ref, own_ref, near_ref = take(3)
        out_ref, moved_ref, told_ref = take(3)
    else:
        asks, own_ref, near_ref, moved_ref, terms_ref = take(5)
        out_ref, whole_ref = take(2)
    groups = take(nz)
    picks, relays, landing = take(3)
    zs, zr, ys, yr, cs, cr, xs, xr, ls = take(9)
    if first or fuse:
        (moved,) = take(1)
    if fuse:
        near, = take(1)
    if first:
        passing, tossed, table, asks = take(4)
        ts, tr, us, ur, js, jr, ms = take(7)
    else:
        cut, stack, pile, joined, ps, pr = take(6)
    own = own_ref.shape[0]
    half = own // 2
    x, z, y, c = (lax.axis_index(a) for a in (AX, AZ, AY, AC))
    east, west = {AX: (x + 1) % nx}, {AX: (x + nx - 1) % nx}
    up, down = {AZ: (z + 1) % nz}, {AZ: (z + nz - 1) % nz}
    fore, back = {AY: (y + 1) % ny}, {AY: (y + ny - 1) % ny}
    mate = {AC: 1 - c}

    def part(j, away, core, start=0, count=own):
        line = (y + away + ny) % ny
        return groups[j].at[pl.ds((line * 2 + core) * own + start, count)]

    def mine(j):
        return own_ref if j == 0 else part(j, 0, c)

    def along_z(j):
        if j <= nz // 2:
            return copy_to(mine(j - 1), part(j, 0, c), zs, zr, j, up)
        return copy_to(mine((j + 1) % nz), part(j, 0, c), zs, zr, j, down)

    def along_y(j, kind):
        if kind == 2:
            piece = part(j, -1, c, 0, half)
            return copy_to(piece, piece, ys, yr, (j, 2), fore)
        if kind == 3:
            piece = part(j, 1, c, half, half)
            return copy_to(piece, piece, ys, yr, (j, 3), back)
        start = 0 if kind in (0, 5) else half
        source = own_ref.at[pl.ds(start, half)] if j == 0 else part(j, 0, c, start, half)
        where = fore if kind in (0, 4) else back
        return copy_to(source, part(j, 0, c, start, half), ys, yr, (j, kind), where)

    def landed_y(j, kind):
        away = (-1, 1, 2, 2, -1, 1)[kind]
        piece = part(j, away, c, 0 if kind in (0, 2, 5) else half, half)
        copy_to(piece, piece, ys, yr, (j, kind), fore).wait_recv()

    def to_mate(j, kind):
        away = (0, -1, 1, 2)[kind]
        source = mine(j) if kind == 0 else part(j, away, c)
        return copy_to(source, part(j, away, c), cs, cr, (j, kind), mate)

    def landed_mate(j, kind):
        piece = part(j, (0, -1, 1, 2)[kind], 1 - c)
        copy_to(piece, piece, cs, cr, (j, kind), mate).wait_recv()

    def far(j):
        return (z + nz - j) % nz

    def row(away):
        return (x + away + nx) % nx

    def along_x(j, kind):
        if kind == 0:
            return copy_to(picks.at[j, pl.ds(0, 4)], landing.at[x, far(j)], xs, xr, (j, 0), east)
        if kind == 1:
            return copy_to(picks.at[j, pl.ds(4, 4)], landing.at[x, far(j)], xs, xr, (j, 1), west)
        if kind == 2:
            return copy_to(picks.at[j, pl.ds(8, 2)], relays.at[j, 0], xs, xr, (j, 2), east)
        if kind == 3:
            return copy_to(picks.at[j, pl.ds(10, 2)], relays.at[j, 1], xs, xr, (j, 3), west)
        if kind == 4:
            place = landing.at[row(-1), far(j), pl.ds(0, 2)]
            return copy_to(relays.at[j, 0], place, xs, xr, (j, 4), east)
        place = landing.at[row(1), far(j), pl.ds(2, 2)]
        return copy_to(relays.at[j, 1], place, xs, xr, (j, 5), west)

    def landed_x(j, kind):
        if kind == 0:
            piece = landing.at[row(-1), far(j)]
        elif kind == 1:
            piece = landing.at[row(1), far(j)]
        elif kind in (2, 3):
            piece = relays.at[j, kind - 2]
        elif kind == 4:
            piece = landing.at[row(2), far(j), pl.ds(0, 2)]
        else:
            piece = landing.at[row(2), far(j), pl.ds(2, 2)]
        copy_to(piece, piece, xs, xr, (j, kind), east).wait_recv()

    def tiles_z(d):
        there = (z + d) % nz
        return copy_to(near_ref.at[:, there], passing.at[d], ts, tr, d, {AZ: there})

    def tiles_for(j, away):
        return near_ref.at[row(away), z] if j == 0 else passing.at[j, row(away)]

    def tiles_x(j, kind):
        if kind == 0:
            return copy_to(tiles_for(j, 1), moved.at[x, far(j)], us, ur, (j, 0), east)
        if kind == 1:
            return copy_to(tiles_for(j, -1), moved.at[x, far(j)], us, ur, (j, 1), west)
        if kind == 2:
            return copy_to(tiles_for(j, 2).at[0], tossed.at[j, 0], us, ur, (j, 2), east)
        if kind == 3:
            return copy_to(tiles_for(j, 2).at[1], tossed.at[j, 1], us, ur, (j, 3), west)
        if kind == 4:
            return copy_to(tossed.at[j, 0], moved.at[row(-1), far(j), 0], us, ur, (j, 4), east)
        return copy_to(tossed.at[j, 1], moved.at[row(1), far(j), 1], us, ur, (j, 5), west)

    def landed_tiles(j, kind):
        if kind == 0:
            piece = moved.at[row(-1), far(j)]
        elif kind == 1:
            piece = moved.at[row(1), far(j)]
        elif kind in (2, 3):
            piece = tossed.at[j, kind - 2]
        elif kind == 4:
            piece = moved.at[row(2), far(j), 0]
        else:
            piece = moved.at[row(2), far(j), 1]
        copy_to(piece, piece, us, ur, (j, kind), east).wait_recv()

    def ids_z(d):
        return copy_to(ids_ref, table.at[x, z], js, jr, d, {AZ: (z + d) % nz})

    def ids_x(d):
        return copy_to(table.at[x], table.at[x], js, jr, nz + d, {AX: (x + d) % nx})

    kept_tiles = lambda: pltpu.make_async_copy(near_ref.at[x, z], moved.at[x, z], ls.at[0])
    all_near = lambda: pltpu.make_async_copy(near_ref, near, ls.at[1])
    all_moved = lambda: pltpu.make_async_copy(moved_ref, moved, ls.at[2])
    all_asks = lambda: pltpu.make_async_copy(table, asks, ls.at[3])

    def results(j):
        return pltpu.make_async_copy(landing.at[:, far(j)], out_ref.at[:, far(j)], ls.at[4 + j])

    def moved_out(j):
        return pltpu.make_async_copy(moved.at[:, far(j)], moved_ref.at[:, far(j)], ms.at[j])

    nsub = 2 * ny
    sub = y * 2 + c

    def sub_place(d):
        there = (sub + d) % nsub
        return {AY: there // 2, AC: there % 2}

    def term(stage, d):
        if stage == 0:
            source = terms_ref.at[(sub + d) % nsub]
            return copy_to(source, cut.at[sub], ps, pr, d, sub_place(d))
        if stage == 1:
            return copy_to(stack.at[z], stack.at[z], ps, pr, nsub + d, {AZ: (z + d) % nz})
        at = nsub + nz + d
        if stage == 2:
            return copy_to(pile.at[x], pile.at[x], ps, pr, at, {AX: (x + d) % nx})
        return copy_to(joined.at[sub], joined.at[sub], ps, pr, at + nx, sub_place(d))

    def term_landed(stage, d):
        back_by = lambda me, count: (me + count - d) % count
        if stage == 0:
            piece, at = cut.at[back_by(sub, nsub)], d
        elif stage == 1:
            piece, at = stack.at[back_by(z, nz)], nsub + d
        elif stage == 2:
            piece, at = pile.at[back_by(x, nx)], nsub + nz + d
        else:
            piece, at = joined.at[back_by(sub, nsub)], nsub + nz + nx + d
        copy_to(piece, piece, ps, pr, at, mate).wait_recv()

    def terms_in(stage):
        return range(1, (nsub, nz, nx, nsub)[stage])

    def send_terms(stage):
        for d in terms_in(stage):
            term(stage, d).start()

    def sum_terms(stage):
        for d in terms_in(stage):
            term_landed(stage, d)
        source, count = ((cut, nsub), (stack, nz), (pile, nx))[stage]
        total = source[0]
        for k in range(1, count):
            total = total + source[k]
        if stage == 0:
            stack[z] = total
        elif stage == 1:
            pile[x] = total
        else:
            joined[sub] = total

    order = visiting_order(nz)
    here = {0}

    def await_z(j):
        if j not in here:
            here.add(j)
            along_z(j).wait_recv()

    def z_step(k):
        for j, step in ((k, 1), (nz - k, -1)):
            ahead = j + step
            if k == 0:
                j, ahead = 0, (1 if step == 1 else nz - 1)
            if step == 1 and ahead > nz // 2 or step == -1 and ahead <= nz // 2:
                continue
            await_z(j)
            along_z(ahead).start()

    def tile_step(k):
        if first and k <= nz // 2:
            for d in sorted({k, nz - k}):
                tiles_z(d).start()

    def spread(j):
        await_z(j)
        for kind in (0, 1, 4, 5):
            along_y(j, kind).start()
        to_mate(j, 0).start()

    def pass_first(j):
        landed_y(j, 0)
        along_y(j, 2).start()
        landed_y(j, 1)
        along_y(j, 3).start()

    def pass_on(j):
        landed_y(j, 4)
        to_mate(j, 1).start()
        landed_y(j, 5)
        to_mate(j, 2).start()
        landed_y(j, 2)
        landed_y(j, 3)
        to_mate(j, 3).start()

    def pick(j):
        for kind in range(4):
            landed_mate(j, kind)

        def asked(away, slot, late):
            line = row(away)
            if late:
                return asks[x, far(j), 0, (line * nz + z) * CAP + slot]
            return asks[line, z, 0, nx * nz * CAP + (x * nz + far(j)) * CAP + slot]

        def one(slot, carry):
            for late in range(2):
                place = late * CAP + slot
                picks[j, place] = groups[j][asked(1, slot, late)]
                picks[j, 4 + place] = groups[j][asked(-1, slot, late)]
                picks[j, 8 + place] = groups[j][asked(2, slot, late)]
                landing[x, far(j), place] = groups[j][asked(0, slot, late)]
            return carry

        lax.fori_loop(0, CAP, one, 0)

    def answer(j):
        for kind in (2, 3, 0, 1):
            along_x(j, kind).start()
        if first and j:
            tiles_z(j).wait_recv()
            moved[x, far(j)] = passing[j, x]
            for kind in (2, 3, 0, 1):
                tiles_x(j, kind).start()

    def relay(j):
        for kind in (2, 3):
            landed_x(j, kind)
            along_x(j, kind + 2).start()
        if first:
            for kind in (2, 3):
                landed_tiles(j, kind)
                tiles_x(j, kind + 2).start()

    def finish(j):
        for kind in (0, 1, 4, 5):
            landed_x(j, kind)
            if first:
                landed_tiles(j, kind)
        if fuse:

            def one(line, carry):
                for slot in range(CAP):
                    value = landing[line, far(j), slot]
                    landing[line, far(j), slot] = product(near[line, far(j), slot], value, False)
                    value = landing[line, far(j), CAP + slot]
                    tile = moved[line, far(j), slot]
                    landing[line, far(j), CAP + slot] = product(tile, value, True)
                return carry

            lax.fori_loop(0, nx, one, 0)
        results(j).start()
        if first:
            moved_out(j).start()

    places = [east, west, up, down, fore, back, mate]
    if first:
        places += [{AX: (x + 2) % nx}] + [{AZ: (z + d) % nz} for d in range(2, nz - 1)]
    else:
        places = [{AX: (x + d) % nx} for d in range(1, nx)]
        places += [{AZ: (z + d) % nz} for d in range(1, nz)]
        places += [sub_place(d) for d in range(1, nsub)]
    greet(places)
    if not first:
        send_terms(0)
    if first:
        for d in range(1, nz):
            ids_z(d).start()
        for kind in (2, 3, 0, 1):
            tiles_x(0, kind).start()
    z_step(0)
    spread(0)
    if first:
        kept_tiles().start()
        table[x, z] = ids_ref[...]
    elif fuse:
        all_moved().start()
        cut[sub] = terms_ref[sub]
    if fuse:
        all_near().start()
    groups[0][pl.ds((y * 2 + c) * own, own)] = own_ref[...]
    pass_first(0)
    spread(order[1])
    z_step(1)
    tile_step(1)
    if first:
        for d in range(1, nz):
            copy_to(table.at[x, far(d)], table.at[x, far(d)], js, jr, d, up).wait_recv()
        for d in range(1, nx):
            ids_x(d).start()
    stages = (1, 2, 5)
    for n, j in enumerate(order):
        if n:
            pass_first(j)
        pass_on(j)
        if n == 0:
            if first:
                kept_tiles().wait()
                for d in range(1, nx):
                    copy_to(table.at[row(-d)], table.at[row(-d)], js, jr, nz + d, east).wait_recv()
                all_asks().start()
                all_asks().wait()
            elif fuse:
                all_moved().wait()
            if fuse:
                all_near().wait()
        pick(j)
        if not first and n in stages:
            sum_terms(stages.index(n))
        if n + 2 < nz:
            spread(order[n + 2])
        if n + 2 < nz // 2:
            z_step(n + 2)
        if n == 1:
            for k in range(3, nz // 2 + 1):
                tile_step(k)
        elif n == 0:
            tile_step(2)
        if n:
            relay(order[n - 1])
        if not first and n in stages:
            send_terms(stages.index(n) + 1)
        answer(j)
        if n > 1:
            finish(order[n - 2])
    relay(order[-1])
    finish(order[-2])
    finish(order[-1])
    if first:
        told_ref[...] = table[...]
    else:
        for d in terms_in(3):
            term_landed(3, d)
        whole_ref[...] = joined[...]
        for stage in range(4):
            for d in terms_in(stage):
                term(stage, d).wait_send()
    for j in order:
        results(j).wait()
        if j:
            along_z(j).wait_send()
        for kind in range(4):
            to_mate(j, kind).wait_send()
        for kind in range(6):
            along_y(j, kind).wait_send()
            along_x(j, kind).wait_send()
        if first:
            moved_out(j).wait()
            for kind in range(6):
                tiles_x(j, kind).wait_send()
            if j:
                tiles_z(j).wait_send()
                ids_z(j).wait_send()
    if first:
        for d in range(1, nx):
            ids_x(d).wait_send()


FUSE = True


def pull(sizes, asks, value, near, moved=None, terms=None):
    nx, nz, ny = sizes
    first = moved is None
    own, rows, width = value.shape
    block = (rows, width)
    dma = pltpu.SemaphoreType.DMA
    tiles = (nx, nz, CAP, rows, rows)
    values = (nx, nz, 2 * CAP, *block)
    anywhere, vmem = pl.BlockSpec(memory_space=pl.ANY), pl.BlockSpec(memory_space=pltpu.VMEM)
    smem = pl.BlockSpec(memory_space=pltpu.SMEM)
    out_shape = [jax.ShapeDtypeStruct(values, F32)]
    out_specs = [anywhere]
    in_specs = [smem, vmem, anywhere, anywhere, vmem]
    scratch = [pltpu.VMEM((ny * 2 * own, *block), F32) for _ in range(nz)] + [
        pltpu.VMEM((nz, 12, *block), F32),
        pltpu.VMEM((nz, 2, 2, *block), F32),
        pltpu.VMEM(values, F32),
        dma((nz,)),
        dma((nz,)),
        dma((nz, 6)),
        dma((nz, 6)),
        dma((nz, 4)),
        dma((nz, 4)),
        dma((nz, 6)),
        dma((nz, 6)),
        dma((4 + nz,)),
    ]
    operands = [asks, value, near, moved, terms]
    if first or FUSE:
        scratch += [pltpu.VMEM(tiles, F32)]
    if FUSE:
        scratch += [pltpu.VMEM(tiles, F32)]
    if first:
        in_specs = [vmem, vmem, anywhere]
        operands = operands[:3]
        told = (nx, nz, *asks.shape)
        out_shape += [jax.ShapeDtypeStruct(tiles, F32), jax.ShapeDtypeStruct(told, jnp.int32)]
        out_specs += [anywhere, vmem]
        scratch += [
            pltpu.VMEM((nz, nx, CAP, rows, rows), F32),
            pltpu.VMEM((nz, 2, rows, rows), F32),
            pltpu.VMEM(told, jnp.int32),
            pltpu.SMEM(told, jnp.int32),
            dma((nz,)),
            dma((nz,)),
            dma((nz, 6)),
            dma((nz, 6)),
            dma((nz + nx,)),
            dma((nz + nx,)),
            dma((nz,)),
        ]
    else:
        out_shape += [jax.ShapeDtypeStruct(terms.shape, F32)]
        out_specs += [vmem]
        scratch += [
            pltpu.VMEM(terms.shape, F32),
            pltpu.VMEM((nz, *terms.shape[1:]), F32),
            pltpu.VMEM((nx, *terms.shape[1:]), F32),
            pltpu.VMEM(terms.shape, F32),
            dma((4 * ny + nz + nx,)),
            dma((4 * ny + nz + nx,)),
        ]
    return pl.pallas_call(
        functools.partial(pull_kernel, sizes, first, FUSE),
        out_shape=out_shape,
        in_specs=in_specs,
        out_specs=out_specs,
        scratch_shapes=scratch,
        compiler_params=pltpu.CompilerParams(
            collective_id=0 if first else 2,
            has_side_effects=True,
            vmem_limit_bytes=58 * 2**20,
        ),
        cost_estimate=pl.CostEstimate(
            flops=20_000_000_000, bytes_accessed=17_000_000, transcendentals=0
        ),
        name="pull_first" if first else "pull_again",
    )(*operands)


def scatter_kernel(ny, sums, out_ref, mated, total, early, late, cs, cr, ys, yr):
    own = out_ref.shape[0]
    half = own // 2
    y, c = lax.axis_index(AY), lax.axis_index(AC)
    fore, back, mate = {AY: (y + 1) % ny}, {AY: (y + ny - 1) % ny}, {AC: 1 - c}

    def at(away, core):
        return pl.ds((((y + away) % ny) * 2 + core) * own, own)

    def over(k):
        return copy_to(sums.at[at(k, 1 - c)], mated.at[k], cs, cr, k, mate)

    early_fore = copy_to(total.at[2, pl.ds(0, half)], early.at[0], ys, yr, 0, fore)
    early_back = copy_to(total.at[2, pl.ds(half, half)], early.at[1], ys, yr, 1, back)


    def late_copy(k, which, where):
        piece = pl.ds((0 if which == k else half), half)
        return copy_to(total.at[2 * k + 1, piece], late.at[k, piece], ys, yr, 2 + 2 * k + which, where)

    late_fore, late_back = ([late_copy(k, w, (fore, back)[k]) for w in (0, 1)] for k in (0, 1))
    greet((fore, back, mate))
    for k in (2, 1, 3, 0):
        over(k).start()
    for k in (2, 1, 3, 0):
        over(k).wait_recv()
        total[k] = sums[at(k, c)] + mated[k]
        if k == 1:
            early_fore.start()
            early_back.start()
        if k == 3:
            late_fore[1].start()
        if k == 0:
            late_back[1].start()
    early_fore.wait_recv()
    total[1, pl.ds(0, half)] = total[1, pl.ds(0, half)] + early[0]
    early_back.wait_recv()
    total[3, pl.ds(half, half)] = total[3, pl.ds(half, half)] + early[1]
    late_fore[0].start()
    late_back[0].start()
    for copy in late_fore + late_back:
        copy.wait_recv()
    out_ref[...] = total[0] + late[0] + late[1]
    for k in range(4):
        over(k).wait_send()
    for copy in [early_fore, early_back] + late_fore + late_back:
        copy.wait_send()


def scatter(ny, sums):
    count, rows, width = sums.shape
    own = count // (2 * ny)
    dma = pltpu.SemaphoreType.DMA
    piece = (own, rows, width)
    return pl.pallas_call(
        functools.partial(scatter_kernel, ny),
        out_shape=jax.ShapeDtypeStruct(piece, F32),
        in_specs=[pl.BlockSpec(memory_space=pltpu.VMEM)],
        out_specs=pl.BlockSpec(memory_space=pltpu.VMEM),
        scratch_shapes=[
            pltpu.VMEM((4, *piece), F32),
            pltpu.VMEM((4, *piece), F32),
            pltpu.VMEM((2, own // 2, rows, width), F32),
            pltpu.VMEM((2, *piece), F32),
            dma((4,)),
            dma((4,)),
            dma((6,)),
            dma((6,)),
        ],
        compiler_params=pltpu.CompilerParams(
            collective_id=1, has_side_effects=True, vmem_limit_bytes=16 * 2**20
        ),
        cost_estimate=pl.CostEstimate(
            flops=2_000_000_000, bytes_accessed=2_000_000, transcendentals=0
        ),
        name="scatter",
    )(sums)


def halves(value):
    high = value.astype(jnp.bfloat16)
    return high, (value - high.astype(F32)).astype(jnp.bfloat16)


def product(tile, value, flipped):
    dims = (((0 if flipped else 1,), (0,)), ((), ()))
    tile_high, tile_low = halves(tile)
    high, low = halves(value)

    def dot(a, b):
        return lax.dot_general(a, b, dims, preferred_element_type=F32)

    return dot(tile_high, high) + (dot(tile_high, low) + dot(tile_low, high))


def add_kernel(step, group, told, products, sums, total):
    first = pl.program_id(0) * step
    count = pl.num_programs(0) * step * CAP
    me = group[0]

    spare = sums.shape[0]

    @pl.when(first == 0)
    def _():
        total[...] = jnp.zeros_like(total)

    for g in range(step):
        for slot in range(2 * CAP):
            if slot < CAP:
                at = me * (4 * count) + (first + g) * CAP + slot
                alive, target = told[at + 2 * count], told[at]
            else:
                at = (first + g) * (4 * count) + me * CAP + slot - CAP
                alive, target = told[at + 2 * count], told[at + count]

            target = jnp.where(alive > 0, target, spare)
            total[target] += products[g, slot]

    @pl.when(pl.program_id(0) == pl.num_programs(0) - 1)
    def _():
        sums[...] = total[pl.ds(0, spare)]


def add(group_size, group, told, products):
    count, slots, rows, width = products.shape
    step = 4
    return pl.pallas_call(
        functools.partial(add_kernel, step),
        out_shape=jax.ShapeDtypeStruct((group_size, rows, width), F32),
        grid_spec=pltpu.PrefetchScalarGridSpec(
            num_scalar_prefetch=2,
            grid=(count // step,),
            in_specs=[pl.BlockSpec((step, slots, rows, width), lambda n, *_: (n, 0, 0, 0))],
            out_specs=pl.BlockSpec((group_size, rows, width), lambda n, *_: (0, 0, 0)),
            scratch_shapes=[pltpu.VMEM((group_size + 1, rows, width), F32)],
        ),
        compiler_params=pltpu.CompilerParams(vmem_limit_bytes=58 * 2**20),
        cost_estimate=pl.CostEstimate(
            flops=count * slots * rows * width, bytes_accessed=11_000_000, transcendentals=0
        ),
        name="add",
    )(group, told, products)


def body(features, weight, bias, adj_tiles, tile_rows, tile_cols, tile_counts, cotangent):
    nx, nz, ny = (lax.axis_size(a) for a in (AX, AZ, AY))
    sizes = (nx, nz, ny)
    blocks = nx * nz
    rows, width = adj_tiles.shape[1], features.shape[1]
    own = features.shape[0] // rows
    group_size = own * ny * 2
    group = lax.axis_index(BLK)
    scale = 1.0 / math.sqrt(features.shape[0] * blocks * ny * 2)
    slots = jnp.arange(blocks * CAP, dtype=jnp.int32)
    alive = (slots % CAP < tile_counts[slots // CAP]).astype(jnp.int32)
    row_local = tile_rows - group * group_size
    col_local = tile_cols - slots // CAP * group_size
    ids = jnp.concatenate([row_local, col_local, alive, alive]).reshape(2, -1)
    near = adj_tiles.reshape(nx, nz, CAP, rows, rows)

    def collect(products, asks, shape):
        me = group.astype(jnp.int32).reshape(1)
        products = products.reshape(blocks, 2 * CAP, rows, width)
        return scatter(ny, add(group_size, me, asks.reshape(-1), products)).reshape(shape)

    dot = functools.partial(jnp.dot, precision=lax.Precision.HIGHEST)
    cut = (own, rows, width)
    products, moved, asks = pull(sizes, ids, features.reshape(cut), near)
    spread = collect(products, asks, features.shape)
    pre = dot(spread, weight) + bias
    sigma = jax.nn.sigmoid(pre)
    activation = pre * sigma
    grad_pre = cotangent * sigma * (1.0 + pre * (1.0 - sigma))
    pieces = 2 * ny
    spare = -(weight.shape[0] + 1) % (8 * pieces)
    terms = jnp.concatenate(
        [
            dot(spread.T, grad_pre) * scale,
            jnp.sum(grad_pre, axis=0)[None] * scale,
            jnp.zeros((spare, width), F32),
        ]
    ).reshape(pieces, -1, width)
    products, params = pull(sizes, asks, grad_pre.reshape(cut), near, moved, terms)
    grad_mixed = collect(products, asks, features.shape)
    grad_features = dot(grad_mixed, weight.T)
    params = params.reshape(-1, width)
    return (activation, grad_features, params[: weight.shape[0]], params[weight.shape[0]])


def solution(mesh):
    finer = Mesh(mesh.devices.reshape(4, 8, 4, 2), ALL)
    return jax.shard_map(
        body,
        mesh=finer,
        in_specs=(
            P(ALL, None),
            P(),
            P(),
            P(ALL, None, None),
            P(ALL),
            P(ALL),
            P(ALL),
            P(ALL, None),
        ),
        out_specs=(P(ALL, None), P(ALL, None), P(), P()),
        check_vma=False,
    )
```

```python
import functools
import math

import jax
import jax.numpy as jnp
from jax import lax
from jax.experimental import pallas as pl
from jax.experimental.pallas import tpu as pltpu
from jax.sharding import Mesh
from jax.sharding import PartitionSpec as P

CAP = 2
MESH = pl.DeviceIdType.MESH
AX, AZ, AY, AC = "blk_0", "blk_1", "sub_0", "sub_1"
ALL = (AX, AZ, AY, AC)
BLK = (AX, AZ)
F32 = jnp.float32


def copy_to(src, dst, sends, recvs, at, where):
    return pltpu.make_async_remote_copy(
        src_ref=src,
        dst_ref=dst,
        send_sem=sends.at[at],
        recv_sem=recvs.at[at],
        device_id=where,
        device_id_type=MESH,
    )


def greet(places):
    barrier = pltpu.get_barrier_semaphore()
    for place in places:
        pl.semaphore_signal(barrier, inc=1, device_id=place, device_id_type=MESH)
    pl.semaphore_wait(barrier, len(places))


def visiting_order(count):
    order = [0]
    for step in range(1, count // 2 + 1):
        order.append(step)
        if count - step > count // 2:
            order.append(count - step)
    return order


def pull_kernel(sizes, first, fuse, *refs):
    nx, nz, ny = sizes
    refs = list(refs)

    def take(count):
        taken, refs[:count] = refs[:count], []
        return taken

    if first:
        ids_ref, own_ref, near_ref = take(3)
        out_ref, moved_ref, told_ref = take(3)
    else:
        asks, own_ref, near_ref, moved_ref, terms_ref = take(5)
        out_ref, whole_ref = take(2)
    groups = take(nz)
    picks, relays, landing = take(3)
    zs, zr, ys, yr, cs, cr, xs, xr, ls = take(9)
    if first or fuse:
        (moved,) = take(1)
    if fuse:
        near, = take(1)
    if first:
        passing, tossed, table, asks = take(4)
        ts, tr, us, ur, js, jr, ms = take(7)
    else:
        cut, stack, pile, joined, ps, pr = take(6)
    own = own_ref.shape[0]
    half = own // 2
    x, z, y, c = (lax.axis_index(a) for a in (AX, AZ, AY, AC))
    east, west = {AX: (x + 1) % nx}, {AX: (x + nx - 1) % nx}
    up, down = {AZ: (z + 1) % nz}, {AZ: (z + nz - 1) % nz}
    fore, back = {AY: (y + 1) % ny}, {AY: (y + ny - 1) % ny}
    mate = {AC: 1 - c}

    def part(j, away, core, start=0, count=own):
        line = (y + away + ny) % ny
        return groups[j].at[pl.ds((line * 2 + core) * own + start, count)]

    def mine(j):
        return own_ref if j == 0 else part(j, 0, c)

    def along_z(j):
        if j <= nz // 2:
            return copy_to(mine(j - 1), part(j, 0, c), zs, zr, j, up)
        return copy_to(mine((j + 1) % nz), part(j, 0, c), zs, zr, j, down)

    def along_y(j, kind):
        if kind == 2:
            piece = part(j, -1, c, 0, half)
            return copy_to(piece, piece, ys, yr, (j, 2), fore)
        if kind == 3:
            piece = part(j, 1, c, half, half)
            return copy_to(piece, piece, ys, yr, (j, 3), back)
        start = 0 if kind in (0, 5) else half
        source = own_ref.at[pl.ds(start, half)] if j == 0 else part(j, 0, c, start, half)
        where = fore if kind in (0, 4) else back
        return copy_to(source, part(j, 0, c, start, half), ys, yr, (j, kind), where)

    def landed_y(j, kind):
        away = (-1, 1, 2, 2, -1, 1)[kind]
        piece = part(j, away, c, 0 if kind in (0, 2, 5) else half, half)
        copy_to(piece, piece, ys, yr, (j, kind), fore).wait_recv()

    def to_mate(j, kind):
        away = (0, -1, 1, 2)[kind]
        source = mine(j) if kind == 0 else part(j, away, c)
        return copy_to(source, part(j, away, c), cs, cr, (j, kind), mate)

    def landed_mate(j, kind):
        piece = part(j, (0, -1, 1, 2)[kind], 1 - c)
        copy_to(piece, piece, cs, cr, (j, kind), mate).wait_recv()

    def far(j):
        return (z + nz - j) % nz

    def row(away):
        return (x + away + nx) % nx

    def along_x(j, kind):
        if kind == 0:
            return copy_to(picks.at[j, pl.ds(0, 4)], landing.at[x, far(j)], xs, xr, (j, 0), east)
        if kind == 1:
            return copy_to(picks.at[j, pl.ds(4, 4)], landing.at[x, far(j)], xs, xr, (j, 1), west)
        if kind == 2:
            return copy_to(picks.at[j, pl.ds(8, 2)], relays.at[j, 0], xs, xr, (j, 2), east)
        if kind == 3:
            return copy_to(picks.at[j, pl.ds(10, 2)], relays.at[j, 1], xs, xr, (j, 3), west)
        if kind == 4:
            place = landing.at[row(-1), far(j), pl.ds(0, 2)]
            return copy_to(relays.at[j, 0], place, xs, xr, (j, 4), east)
        place = landing.at[row(1), far(j), pl.ds(2, 2)]
        return copy_to(relays.at[j, 1], place, xs, xr, (j, 5), west)

    def landed_x(j, kind):
        if kind == 0:
            piece = landing.at[row(-1), far(j)]
        elif kind == 1:
            piece = landing.at[row(1), far(j)]
        elif kind in (2, 3):
            piece = relays.at[j, kind - 2]
        elif kind == 4:
            piece = landing.at[row(2), far(j), pl.ds(0, 2)]
        else:
            piece = landing.at[row(2), far(j), pl.ds(2, 2)]
        copy_to(piece, piece, xs, xr, (j, kind), east).wait_recv()

    def tiles_z(d):
        there = (z + d) % nz
        return copy_to(near_ref.at[:, there], passing.at[d], ts, tr, d, {AZ: there})

    def tiles_for(j, away):
        return near_ref.at[row(away), z] if j == 0 else passing.at[j, row(away)]

    def tiles_x(j, kind):
        if kind == 0:
            return copy_to(tiles_for(j, 1), moved.at[x, far(j)], us, ur, (j, 0), east)
        if kind == 1:
            return copy_to(tiles_for(j, -1), moved.at[x, far(j)], us, ur, (j, 1), west)
        if kind == 2:
            return copy_to(tiles_for(j, 2).at[0], tossed.at[j, 0], us, ur, (j, 2), east)
        if kind == 3:
            return copy_to(tiles_for(j, 2).at[1], tossed.at[j, 1], us, ur, (j, 3), west)
        if kind == 4:
            return copy_to(tossed.at[j, 0], moved.at[row(-1), far(j), 0], us, ur, (j, 4), east)
        return copy_to(tossed.at[j, 1], moved.at[row(1), far(j), 1], us, ur, (j, 5), west)

    def landed_tiles(j, kind):
        if kind == 0:
            piece = moved.at[row(-1), far(j)]
        elif kind == 1:
            piece = moved.at[row(1), far(j)]
        elif kind in (2, 3):
            piece = tossed.at[j, kind - 2]
        elif kind == 4:
            piece = moved.at[row(2), far(j), 0]
        else:
            piece = moved.at[row(2), far(j), 1]
        copy_to(piece, piece, us, ur, (j, kind), east).wait_recv()

    def ids_z(d):
        return copy_to(ids_ref, table.at[x, z], js, jr, d, {AZ: (z + d) % nz})

    def ids_x(d):
        return copy_to(table.at[x], table.at[x], js, jr, nz + d, {AX: (x + d) % nx})

    kept_tiles = lambda: pltpu.make_async_copy(near_ref.at[x, z], moved.at[x, z], ls.at[0])
    all_near = lambda: pltpu.make_async_copy(near_ref, near, ls.at[1])
    all_moved = lambda: pltpu.make_async_copy(moved_ref, moved, ls.at[2])
    all_asks = lambda: pltpu.make_async_copy(table, asks, ls.at[3])

    def results(j):
        return pltpu.make_async_copy(landing.at[:, far(j)], out_ref.at[:, far(j)], ls.at[4 + j])

    def moved_out(j):
        return pltpu.make_async_copy(moved.at[:, far(j)], moved_ref.at[:, far(j)], ms.at[j])

    nsub = 2 * ny
    sub = y * 2 + c

    def sub_place(d):
        there = (sub + d) % nsub
        return {AY: there // 2, AC: there % 2}

    def term(stage, d):
        if stage == 0:
            source = terms_ref.at[(sub + d) % nsub]
            return copy_to(source, cut.at[sub], ps, pr, d, sub_place(d))
        if stage == 1:
            return copy_to(stack.at[z], stack.at[z], ps, pr, nsub + d, {AZ: (z + d) % nz})
        at = nsub + nz + d
        if stage == 2:
            return copy_to(pile.at[x], pile.at[x], ps, pr, at, {AX: (x + d) % nx})
        return copy_to(joined.at[sub], joined.at[sub], ps, pr, at + nx, sub_place(d))

    def term_landed(stage, d):
        back_by = lambda me, count: (me + count - d) % count
        if stage == 0:
            piece, at = cut.at[back_by(sub, nsub)], d
        elif stage == 1:
            piece, at = stack.at[back_by(z, nz)], nsub + d
        elif stage == 2:
            piece, at = pile.at[back_by(x, nx)], nsub + nz + d
        else:
            piece, at = joined.at[back_by(sub, nsub)], nsub + nz + nx + d
        copy_to(piece, piece, ps, pr, at, mate).wait_recv()

    def terms_in(stage):
        return range(1, (nsub, nz, nx, nsub)[stage])

    def send_terms(stage):
        for d in terms_in(stage):
            term(stage, d).start()

    def sum_terms(stage):
        for d in terms_in(stage):
            term_landed(stage, d)
        source, count = ((cut, nsub), (stack, nz), (pile, nx))[stage]
        total = source[0]
        for k in range(1, count):
            total = total + source[k]
        if stage == 0:
            stack[z] = total
        elif stage == 1:
            pile[x] = total
        else:
            joined[sub] = total

    order = visiting_order(nz)
    here = {0}

    def await_z(j):
        if j not in here:
            here.add(j)
            along_z(j).wait_recv()

    def z_step(k):
        for j, step in ((k, 1), (nz - k, -1)):
            ahead = j + step
            if k == 0:
                j, ahead = 0, (1 if step == 1 else nz - 1)
            if step == 1 and ahead > nz // 2 or step == -1 and ahead <= nz // 2:
                continue
            await_z(j)
            along_z(ahead).start()

    def tile_step(k):
        if first and k <= nz // 2:
            for d in sorted({k, nz - k}):
                tiles_z(d).start()

    def spread(j):
        await_z(j)
        for kind in (0, 1, 4, 5):
            along_y(j, kind).start()
        to_mate(j, 0).start()

    def pass_first(j):
        landed_y(j, 0)
        along_y(j, 2).start()
        landed_y(j, 1)
        along_y(j, 3).start()

    def pass_on(j):
        landed_y(j, 4)
        to_mate(j, 1).start()
        landed_y(j, 5)
        to_mate(j, 2).start()
        landed_y(j, 2)
        landed_y(j, 3)
        to_mate(j, 3).start()

    def pick(j):
        for kind in range(4):
            landed_mate(j, kind)

        def asked(away, slot, late):
            line = row(away)
            if late:
                return asks[x, far(j), 0, (line * nz + z) * CAP + slot]
            return asks[line, z, 0, nx * nz * CAP + (x * nz + far(j)) * CAP + slot]

        def one(slot, carry):
            for late in range(2):
                place = late * CAP + slot
                picks[j, place] = groups[j][asked(1, slot, late)]
                picks[j, 4 + place] = groups[j][asked(-1, slot, late)]
                picks[j, 8 + place] = groups[j][asked(2, slot, late)]
                landing[x, far(j), place] = groups[j][asked(0, slot, late)]
            return carry

        lax.fori_loop(0, CAP, one, 0)

    def answer(j):
        for kind in (2, 3, 0, 1):
            along_x(j, kind).start()
        if first and j:
            tiles_z(j).wait_recv()
            moved[x, far(j)] = passing[j, x]
            for kind in (2, 3, 0, 1):
                tiles_x(j, kind).start()

    def relay(j):
        for kind in (2, 3):
            landed_x(j, kind)
            along_x(j, kind + 2).start()
        if first:
            for kind in (2, 3):
                landed_tiles(j, kind)
                tiles_x(j, kind + 2).start()

    def finish(j):
        for kind in (0, 1, 4, 5):
            landed_x(j, kind)
            if first:
                landed_tiles(j, kind)
        if fuse:

            def one(line, carry):
                for slot in range(CAP):
                    value = landing[line, far(j), slot]
                    landing[line, far(j), slot] = product(near[line, far(j), slot], value, False)
                    value = landing[line, far(j), CAP + slot]
                    tile = moved[line, far(j), slot]
                    landing[line, far(j), CAP + slot] = product(tile, value, True)
                return carry

            lax.fori_loop(0, nx, one, 0)
        results(j).start()
        if first:
            moved_out(j).start()

    places = [east, west, up, down, fore, back, mate]
    if first:
        places += [{AX: (x + 2) % nx}] + [{AZ: (z + d) % nz} for d in range(2, nz - 1)]
    else:
        places = [{AX: (x + d) % nx} for d in range(1, nx)]
        places += [{AZ: (z + d) % nz} for d in range(1, nz)]
        places += [sub_place(d) for d in range(1, nsub)]
    greet(places)
    if not first:
        send_terms(0)
    if first:
        for d in range(1, nz):
            ids_z(d).start()
        for kind in (2, 3, 0, 1):
            tiles_x(0, kind).start()
    z_step(0)
    spread(0)
    if first:
        kept_tiles().start()
        table[x, z] = ids_ref[...]
    elif fuse:
        all_moved().start()
        cut[sub] = terms_ref[sub]
    if fuse:
        all_near().start()
    groups[0][pl.ds((y * 2 + c) * own, own)] = own_ref[...]
    pass_first(0)
    spread(order[1])
    z_step(1)
    tile_step(1)
    if first:
        for d in range(1, nz):
            copy_to(table.at[x, far(d)], table.at[x, far(d)], js, jr, d, up).wait_recv()
        for d in range(1, nx):
            ids_x(d).start()
    stages = (1, 2, 5)
    for n, j in enumerate(order):
        if n:
            pass_first(j)
        pass_on(j)
        if n == 0:
            if first:
                kept_tiles().wait()
                for d in range(1, nx):
                    copy_to(table.at[row(-d)], table.at[row(-d)], js, jr, nz + d, east).wait_recv()
                all_asks().start()
                all_asks().wait()
            elif fuse:
                all_moved().wait()
            if fuse:
                all_near().wait()
        pick(j)
        if not first and n in stages:
            sum_terms(stages.index(n))
        if n + 2 < nz:
            spread(order[n + 2])
        if n + 2 < nz // 2:
            z_step(n + 2)
        if n == 1:
            for k in range(3, nz // 2 + 1):
                tile_step(k)
        elif n == 0:
            tile_step(2)
        if n:
            relay(order[n - 1])
        if not first and n in stages:
            send_terms(stages.index(n) + 1)
        answer(j)
        if n > 1:
            finish(order[n - 2])
    relay(order[-1])
    finish(order[-2])
    finish(order[-1])
    if first:
        told_ref[...] = table[...]
    else:
        for d in terms_in(3):
            term_landed(3, d)
        whole_ref[...] = joined[...]
        for stage in range(4):
            for d in terms_in(stage):
                term(stage, d).wait_send()
    for j in order:
        results(j).wait()
        if j:
            along_z(j).wait_send()
        for kind in range(4):
            to_mate(j, kind).wait_send()
        for kind in range(6):
            along_y(j, kind).wait_send()
            along_x(j, kind).wait_send()
        if first:
            moved_out(j).wait()
            for kind in range(6):
                tiles_x(j, kind).wait_send()
            if j:
                tiles_z(j).wait_send()
                ids_z(j).wait_send()
    if first:
        for d in range(1, nx):
            ids_x(d).wait_send()


FUSE = True


def pull(sizes, asks, value, near, moved=None, terms=None):
    nx, nz, ny = sizes
    first = moved is None
    own, rows, width = value.shape
    block = (rows, width)
    dma = pltpu.SemaphoreType.DMA
    tiles = (nx, nz, CAP, rows, rows)
    values = (nx, nz, 2 * CAP, *block)
    anywhere, vmem = pl.BlockSpec(memory_space=pl.ANY), pl.BlockSpec(memory_space=pltpu.VMEM)
    smem = pl.BlockSpec(memory_space=pltpu.SMEM)
    out_shape = [jax.ShapeDtypeStruct(values, F32)]
    out_specs = [anywhere]
    in_specs = [smem, vmem, anywhere, anywhere, vmem]
    scratch = [pltpu.VMEM((ny * 2 * own, *block), F32) for _ in range(nz)] + [
        pltpu.VMEM((nz, 12, *block), F32),
        pltpu.VMEM((nz, 2, 2, *block), F32),
        pltpu.VMEM(values, F32),
        dma((nz,)),
        dma((nz,)),
        dma((nz, 6)),
        dma((nz, 6)),
        dma((nz, 4)),
        dma((nz, 4)),
        dma((nz, 6)),
        dma((nz, 6)),
        dma((4 + nz,)),
    ]
    operands = [asks, value, near, moved, terms]
    if first or FUSE:
        scratch += [pltpu.VMEM(tiles, F32)]
    if FUSE:
        scratch += [pltpu.VMEM(tiles, F32)]
    if first:
        in_specs = [vmem, vmem, anywhere]
        operands = operands[:3]
        told = (nx, nz, *asks.shape)
        out_shape += [jax.ShapeDtypeStruct(tiles, F32), jax.ShapeDtypeStruct(told, jnp.int32)]
        out_specs += [anywhere, vmem]
        scratch += [
            pltpu.VMEM((nz, nx, CAP, rows, rows), F32),
            pltpu.VMEM((nz, 2, rows, rows), F32),
            pltpu.VMEM(told, jnp.int32),
            pltpu.SMEM(told, jnp.int32),
            dma((nz,)),
            dma((nz,)),
            dma((nz, 6)),
            dma((nz, 6)),
            dma((nz + nx,)),
            dma((nz + nx,)),
            dma((nz,)),
        ]
    else:
        out_shape += [jax.ShapeDtypeStruct(terms.shape, F32)]
        out_specs += [vmem]
        scratch += [
            pltpu.VMEM(terms.shape, F32),
            pltpu.VMEM((nz, *terms.shape[1:]), F32),
            pltpu.VMEM((nx, *terms.shape[1:]), F32),
            pltpu.VMEM(terms.shape, F32),
            dma((4 * ny + nz + nx,)),
            dma((4 * ny + nz + nx,)),
        ]
    return pl.pallas_call(
        functools.partial(pull_kernel, sizes, first, FUSE),
        out_shape=out_shape,
        in_specs=in_specs,
        out_specs=out_specs,
        scratch_shapes=scratch,
        compiler_params=pltpu.CompilerParams(
            collective_id=0 if first else 2,
            has_side_effects=True,
            vmem_limit_bytes=58 * 2**20,
        ),
        cost_estimate=pl.CostEstimate(
            flops=20_000_000_000, bytes_accessed=17_000_000, transcendentals=0
        ),
        name="pull_first" if first else "pull_again",
    )(*operands)


def scatter_kernel(ny, sums, out_ref, mated, total, early, late, cs, cr, ys, yr):
    own = out_ref.shape[0]
    half = own // 2
    y, c = lax.axis_index(AY), lax.axis_index(AC)
    fore, back, mate = {AY: (y + 1) % ny}, {AY: (y + ny - 1) % ny}, {AC: 1 - c}

    def at(away, core):
        return pl.ds((((y + away) % ny) * 2 + core) * own, own)

    def over(k):
        return copy_to(sums.at[at(k, 1 - c)], mated.at[k], cs, cr, k, mate)

    early_fore = copy_to(total.at[2, pl.ds(0, half)], early.at[0], ys, yr, 0, fore)
    early_back = copy_to(total.at[2, pl.ds(half, half)], early.at[1], ys, yr, 1, back)


    def late_copy(k, which, where):
        piece = pl.ds((0 if which == k else half), half)
        return copy_to(total.at[2 * k + 1, piece], late.at[k, piece], ys, yr, 2 + 2 * k + which, where)

    late_fore, late_back = ([late_copy(k, w, (fore, back)[k]) for w in (0, 1)] for k in (0, 1))
    greet((fore, back, mate))
    for k in (2, 1, 3, 0):
        over(k).start()
    for k in (2, 1, 3, 0):
        over(k).wait_recv()
        total[k] = sums[at(k, c)] + mated[k]
        if k == 1:
            early_fore.start()
            early_back.start()
        if k == 3:
            late_fore[1].start()
        if k == 0:
            late_back[1].start()
    early_fore.wait_recv()
    total[1, pl.ds(0, half)] = total[1, pl.ds(0, half)] + early[0]
    early_back.wait_recv()
    total[3, pl.ds(half, half)] = total[3, pl.ds(half, half)] + early[1]
    late_fore[0].start()
    late_back[0].start()
    for copy in late_fore + late_back:
        copy.wait_recv()
    out_ref[...] = total[0] + late[0] + late[1]
    for k in range(4):
        over(k).wait_send()
    for copy in [early_fore, early_back] + late_fore + late_back:
        copy.wait_send()


def scatter(ny, sums):
    count, rows, width = sums.shape
    own = count // (2 * ny)
    dma = pltpu.SemaphoreType.DMA
    piece = (own, rows, width)
    return pl.pallas_call(
        functools.partial(scatter_kernel, ny),
        out_shape=jax.ShapeDtypeStruct(piece, F32),
        in_specs=[pl.BlockSpec(memory_space=pltpu.VMEM)],
        out_specs=pl.BlockSpec(memory_space=pltpu.VMEM),
        scratch_shapes=[
            pltpu.VMEM((4, *piece), F32),
            pltpu.VMEM((4, *piece), F32),
            pltpu.VMEM((2, own // 2, rows, width), F32),
            pltpu.VMEM((2, *piece), F32),
            dma((4,)),
            dma((4,)),
            dma((6,)),
            dma((6,)),
        ],
        compiler_params=pltpu.CompilerParams(
            collective_id=1, has_side_effects=True, vmem_limit_bytes=16 * 2**20
        ),
        cost_estimate=pl.CostEstimate(
            flops=2_000_000_000, bytes_accessed=2_000_000, transcendentals=0
        ),
        name="scatter",
    )(sums)


def halves(value):
    high = value.astype(jnp.bfloat16)
    return high, (value - high.astype(F32)).astype(jnp.bfloat16)


def product(tile, value, flipped):
    dims = (((0 if flipped else 1,), (0,)), ((), ()))
    tile_high, tile_low = halves(tile)
    high, low = halves(value)

    def dot(a, b):
        return lax.dot_general(a, b, dims, preferred_element_type=F32)

    return dot(tile_high, high) + (dot(tile_high, low) + dot(tile_low, high))


def add_kernel(group, told, products, sums, total, held, sems):
    count, spare = held.shape[0], sums.shape[0]
    step = count // sems.shape[0]
    me = group[0]

    def piece(k):
        rows = pl.ds(k * step, step)
        return pltpu.make_async_copy(products.at[rows], held.at[rows], sems.at[k])

    for k in range(count // step):
        piece(k).start()
    total[...] = jnp.zeros_like(total)
    for k in range(count // step):
        piece(k).wait()
        for g in range(k * step, k * step + step):
            for slot in range(2 * CAP):
                if slot < CAP:
                    at = me * (4 * CAP * count) + g * CAP + slot
                    alive, target = told[at + 2 * CAP * count], told[at]
                else:
                    at = g * (4 * CAP * count) + me * CAP + slot - CAP
                    alive, target = told[at + 2 * CAP * count], told[at + CAP * count]
                target = jnp.where(alive > 0, target, spare)
                total[target] += held[g, slot]
    sums[...] = total[pl.ds(0, spare)]


def add(group_size, group, told, products):
    count, slots, rows, width = products.shape
    smem = pl.BlockSpec(memory_space=pltpu.SMEM)
    return pl.pallas_call(
        add_kernel,
        out_shape=jax.ShapeDtypeStruct((group_size, rows, width), F32),
        in_specs=[smem, smem, pl.BlockSpec(memory_space=pl.ANY)],
        out_specs=pl.BlockSpec(memory_space=pltpu.VMEM),
        scratch_shapes=[
            pltpu.VMEM((group_size + 1, rows, width), F32),
            pltpu.VMEM(products.shape, F32),
            pltpu.SemaphoreType.DMA((16,)),
        ],
        compiler_params=pltpu.CompilerParams(vmem_limit_bytes=57 * 2**20),
        cost_estimate=pl.CostEstimate(
            flops=count * slots * rows * width, bytes_accessed=11_000_000, transcendentals=0
        ),
        name="add",
    )(group, told, products)


def body(features, weight, bias, adj_tiles, tile_rows, tile_cols, tile_counts, cotangent):
    nx, nz, ny = (lax.axis_size(a) for a in (AX, AZ, AY))
    sizes = (nx, nz, ny)
    blocks = nx * nz
    rows, width = adj_tiles.shape[1], features.shape[1]
    own = features.shape[0] // rows
    group_size = own * ny * 2
    group = lax.axis_index(BLK)
    scale = 1.0 / math.sqrt(features.shape[0] * blocks * ny * 2)
    slots = jnp.arange(blocks * CAP, dtype=jnp.int32)
    alive = (slots % CAP < tile_counts[slots // CAP]).astype(jnp.int32)
    row_local = tile_rows - group * group_size
    col_local = tile_cols - slots // CAP * group_size
    ids = jnp.concatenate([row_local, col_local, alive, alive]).reshape(2, -1)
    near = adj_tiles.reshape(nx, nz, CAP, rows, rows)

    def collect(products, asks, shape):
        me = group.astype(jnp.int32).reshape(1)
        products = products.reshape(blocks, 2 * CAP, rows, width)
        return scatter(ny, add(group_size, me, asks.reshape(-1), products)).reshape(shape)

    dot = functools.partial(jnp.dot, precision=lax.Precision.HIGHEST)
    cut = (own, rows, width)
    products, moved, asks = pull(sizes, ids, features.reshape(cut), near)
    spread = collect(products, asks, features.shape)
    pre = dot(spread, weight) + bias
    sigma = jax.nn.sigmoid(pre)
    activation = pre * sigma
    grad_pre = cotangent * sigma * (1.0 + pre * (1.0 - sigma))
    pieces = 2 * ny
    spare = -(weight.shape[0] + 1) % (8 * pieces)
    terms = jnp.concatenate(
        [
            dot(spread.T, grad_pre) * scale,
            jnp.sum(grad_pre, axis=0)[None] * scale,
            jnp.zeros((spare, width), F32),
        ]
    ).reshape(pieces, -1, width)
    products, params = pull(sizes, asks, grad_pre.reshape(cut), near, moved, terms)
    grad_mixed = collect(products, asks, features.shape)
    grad_features = dot(grad_mixed, weight.T)
    params = params.reshape(-1, width)
    return (activation, grad_features, params[: weight.shape[0]], params[weight.shape[0]])


def solution(mesh):
    finer = Mesh(mesh.devices.reshape(4, 8, 4, 2), ALL)
    return jax.shard_map(
        body,
        mesh=finer,
        in_specs=(
            P(ALL, None),
            P(),
            P(),
            P(ALL, None, None),
            P(ALL),
            P(ALL),
            P(ALL),
            P(ALL, None),
        ),
        out_specs=(P(ALL, None), P(ALL, None), P(), P()),
        check_vma=False,
    )
```
